32 devices in a mesh: px: 16 (over z, x, core), py: 2 (over y).
Axes of the slice: x: 2, y: 2, z: 4, core: 2. Of those that a mesh axis runs over, the one named last changes fastest.
Arguments:
- velocity: float32 [3, 1024, 2, 1024], P(None, 'px', 'py'), may hold values from -1.5 to 2.5
- band_of: int32 [2], replicated, may hold values from 0 to 1, as said below
Outputs:
- correlation: float32 [6, 2, 1024, 1024], P(None, None, ('px', 'py'))
The draws below stay inside these ranges and needn't reach their ends.
Inputs may be any that keep to these rules, and one draw needn't show every extreme that they name: `band_of`: every band 0 to 1 holds at least one plane.
All inputs are finite; a program needn't handle non-finite values.
Results may differ from the reference program's by a relative error of at most 0.00013.
Values sent between devices are 32-bit elements; how exact they have to be, the bound alone decides.
A program may use at most 64 MiB of HBM per device.

```python
import math
import jax
import jax.numpy as jnp
from jax import lax

NX = 1024
NZ = 1024
NY = 2
NB = 2


def draw_band_of(key, part):
    first_key = jax.random.fold_in(key, 11)
    second_key = jax.random.fold_in(key, 23)
    random_band = jax.random.randint(first_key, (NY,), 0, NB, dtype=jnp.int32)
    shuffled = jax.random.permutation(second_key, jnp.arange(NY, dtype=jnp.int32))
    return jnp.where(shuffled < NB, shuffled, random_band).astype(jnp.int32)


def level_of(key, dims, cuts, low, high):
    level, own = 1.0, jax.random.fold_in(key, 6)
    for axis_at, blocks in cuts:
        draws = jnp.exp(jax.random.uniform(jax.random.fold_in(own, axis_at), (blocks,), jnp.float32, low / len(cuts), high / len(cuts)))
        level = level * jnp.repeat(draws, dims[axis_at] // blocks).reshape([-1 if axis == axis_at else 1 for axis in range(len(dims))])
    return level


def setup_inputs(seed: int = 0) -> dict:
    splits = jax.random.split(jax.random.key(seed), 3)
    velocity = jnp.clip(-1.5 + 4.0 * jax.random.uniform(splits[0], (3, NX, NY, NZ), jnp.float32) ** level_of(splits[0], (3, NX, NY, NZ), ((1, 16), (2, 2)), -0.2, 0.2), -1.5, 2.5)
    band_of = draw_band_of(jax.random.fold_in(splits[2], 71), 0)
    return dict(velocity=velocity, band_of=band_of)


PAIR_LIST = ((0, 0), (0, 1), (0, 2), (1, 1), (1, 2), (2, 2))

def reference(velocity, band_of):
    half = NZ // 2
    cells = NX * NZ
    span_spec = jnp.fft.rfft(velocity, axis=3)[..., :half]
    spectrum = jnp.fft.fft(span_spec, axis=1)
    spectrum = spectrum.at[:, 0, :, 0].set(0.0)
    band_ids = jnp.arange(NB, dtype=jnp.int32)
    onehot = (band_of[:, None] == band_ids[None, :]).astype(jnp.float32)
    counts = lax.optimization_barrier(jnp.sum(onehot, 0))
    band_weight = onehot / (counts[None, :] * (cells * math.sqrt(cells)))
    results = []
    for left_comp, right_comp in PAIR_LIST:
        product = jnp.conj(spectrum[left_comp]) * spectrum[right_comp]
        banded_real = jnp.einsum('xyk,yb->bxk', jnp.real(product), band_weight, precision=lax.Precision.HIGHEST)
        banded_imag = jnp.einsum('xyk,yb->bxk', jnp.imag(product), band_weight, precision=lax.Precision.HIGHEST)
        stream_back = jnp.fft.ifft(lax.complex(banded_real, banded_imag), axis=1) * NX
        padded = jnp.concatenate((stream_back, jnp.zeros((NB, NX, 1), stream_back.dtype)), 2)
        results.append(jnp.fft.irfft(padded, n=NZ, axis=2) * NZ)
    return jnp.stack(results, 0)
```

```python
import functools
import math

import jax
import jax.numpy as jnp
import numpy as np
from jax import lax
from jax.experimental import pallas as pl
from jax.experimental.pallas import tpu as pltpu
from jax.sharding import PartitionSpec as P

NB = 2


PAIR_LIST = ((0, 0), (0, 1), (0, 2), (1, 1), (1, 2), (2, 2))


def phase_table(row_values, offset, count, length):
    col_values = offset + lax.iota(jnp.int32, count)
    phase = row_values[:, None] * col_values[None, :] % length
    angle = phase.astype(jnp.float32) * (2.0 * math.pi / length)
    return (jnp.cos(angle), jnp.sin(angle))


def transform_last(real_part, imag_part, sign):
    full_shape = real_part.shape
    length = full_shape[-1]
    stacked = jnp.concatenate((real_part.reshape(-1, length), imag_part.reshape(-1, length)), 0)
    row_count = stacked.shape[0] // 2
    row_values = lax.iota(jnp.int32, length)

    def one_block(block_index, outputs):
        offset = (block_index * 128).astype(jnp.int32)
        cosine_table, sine_table = phase_table(row_values, offset, 128, length)
        with_cos = jnp.dot(
            stacked,
            cosine_table,
            precision=lax.Precision.HIGHEST,
            preferred_element_type=jnp.float32,
        )
        with_sin = jnp.dot(
            stacked, sine_table, precision=lax.Precision.HIGHEST, preferred_element_type=jnp.float32
        )
        new_real = with_cos[:row_count] - sign * with_sin[row_count:]
        new_imag = with_cos[row_count:] + sign * with_sin[:row_count]
        return (
            lax.dynamic_update_slice_in_dim(outputs[0], new_real, offset, 1),
            lax.dynamic_update_slice_in_dim(outputs[1], new_imag, offset, 1),
        )

    zeros = jnp.zeros((row_count, length), jnp.float32)
    out_real, out_imag = lax.fori_loop(0, length // 128, one_block, (zeros, zeros))
    return (out_real.reshape(full_shape), out_imag.reshape(full_shape))


def span_forward(velocity):
    comps, rows_x, planes, length = velocity.shape
    half = length // 2
    row_values = lax.iota(jnp.int32, length)

    def one_block(block_index, outputs):
        offset = (block_index * 128).astype(jnp.int32)
        cosine_table, sine_table = phase_table(row_values, offset, 128, length)
        with_cos = jnp.einsum(
            "cxpz,zk->cpkx",
            velocity,
            cosine_table,
            precision=lax.Precision.HIGHEST,
            preferred_element_type=jnp.float32,
        )
        with_sin = jnp.einsum(
            "cxpz,zk->cpkx",
            velocity,
            sine_table,
            precision=lax.Precision.HIGHEST,
            preferred_element_type=jnp.float32,
        )
        return (
            lax.dynamic_update_slice_in_dim(outputs[0], with_cos, offset, 2),
            lax.dynamic_update_slice_in_dim(outputs[1], -with_sin, offset, 2),
        )

    zeros = jnp.zeros((comps, planes, half, rows_x), jnp.float32)
    return lax.fori_loop(0, half // 128, one_block, (zeros, zeros))


def span_inverse(summed, kz_order):
    half = summed.shape[3]
    length = 2 * half
    multiplier = jnp.where(kz_order == 0, 1.0, 2.0).astype(jnp.float32)
    held_real = summed[:, :, 0] * multiplier[:, None]
    held_imag = summed[:, :, 1] * multiplier[:, None]

    def one_block(block_index, output):
        offset = (block_index * 128).astype(jnp.int32)
        cosine_table, sine_table = phase_table(kz_order, offset, 128, length)
        part = jnp.einsum(
            "sbkd,kz->sbdz",
            held_real,
            cosine_table,
            precision=lax.Precision.HIGHEST,
            preferred_element_type=jnp.float32,
        )
        part = part - jnp.einsum(
            "sbkd,kz->sbdz",
            held_imag,
            sine_table,
            precision=lax.Precision.HIGHEST,
            preferred_element_type=jnp.float32,
        )
        return lax.dynamic_update_slice_in_dim(output, part, offset, 3)

    zeros = jnp.zeros((summed.shape[0], summed.shape[1], summed.shape[4], length), jnp.float32)
    return lax.fori_loop(0, length // 128, one_block, zeros)


def general_device(velocity, band_of):
    px_count = lax.axis_size("px")
    py_count = lax.axis_size("py")
    comps, rows_x, planes, span = velocity.shape
    stream = rows_x * px_count
    half = span // 2
    local_k = half // px_count
    span_real, span_imag = span_forward(velocity)
    planes_spec = jnp.stack((span_real, span_imag), 1)
    kz_index = lax.iota(jnp.int32, local_k)
    kx_index = lax.iota(jnp.int32, stream)
    at_anchor = jnp.logical_and(
        lax.axis_index("px") == 0, jnp.logical_and(kz_index[:, None] == 0, kx_index[None, :] == 0)
    )
    keep_mask = 1.0 - at_anchor.astype(jnp.float32)
    received = lax.all_to_all(planes_spec, "px", split_axis=3, concat_axis=4, tiled=True)
    front_real, front_imag = transform_last(received[:, 0], received[:, 1], -1.0)
    spectrum = jnp.stack((front_real * keep_mask, front_imag * keep_mask), 1)
    cross_list = []
    for left_comp, right_comp in PAIR_LIST:
        left_real, left_imag = (spectrum[left_comp, 0], spectrum[left_comp, 1])
        right_real, right_imag = (spectrum[right_comp, 0], spectrum[right_comp, 1])
        cross_list.append(
            jnp.stack(
                (
                    left_real * right_real + left_imag * right_imag,
                    left_real * right_imag - left_imag * right_real,
                ),
                0,
            )
        )
    cross = jnp.stack(cross_list, 0)
    band_ids = lax.iota(jnp.int32, NB)
    onehot_all = (band_of[:, None] == band_ids[None, :]).astype(jnp.float32)
    counts = jnp.sum(onehot_all, 0)
    cells = float(stream * span)
    plane_start = lax.axis_index("py") * planes
    local_hot = lax.dynamic_slice_in_dim(onehot_all, plane_start, planes, 0)
    band_weight = local_hot / (counts[None, :] * (cells * math.sqrt(cells)))
    banded = jnp.einsum("sapkx,pb->sbakx", cross, band_weight, precision=lax.Precision.HIGHEST)
    summed = lax.psum_scatter(banded, "py", scatter_dimension=3, tiled=True)
    back_real, back_imag = transform_last(summed[:, :, 0], summed[:, :, 1], 1.0)
    exchanged = lax.all_to_all(
        lax.all_to_all(
            jnp.stack((back_real, back_imag), 2), "px", split_axis=4, concat_axis=3, tiled=True
        ),
        "py",
        split_axis=4,
        concat_axis=3,
        tiled=True,
    )
    quarter = local_k // py_count
    position = lax.iota(jnp.int32, half)
    outer = position // (px_count * quarter)
    remain = position % (px_count * quarter)
    kz_order = remain // quarter * local_k + outer * quarter + remain % quarter
    return span_inverse(exchanged, kz_order)


def split_table(table):
    high = table.astype(jnp.bfloat16)
    low = (table - high.astype(np.float64)).astype(jnp.bfloat16)
    return high, low


def span_tables(length):
    quarter, eighth = length // 4, length // 8
    column = np.arange(quarter)

    def angle(first, count):
        wave = 4 * np.arange(count) + first
        return 2.0 * np.pi * ((wave[:, None] * column[None, :]) % length) / length

    even = angle(0, eighth)
    middle = angle(2, eighth)
    odd = angle(1, quarter)
    table_even = np.concatenate((np.cos(even), -np.sin(even)), 0)
    table_middle = np.concatenate((np.cos(middle), -np.sin(middle)), 0)
    table_odd = np.block([[np.cos(odd), -np.sin(odd)], [-np.sin(odd), -np.cos(odd)]])
    return split_table(table_even) + split_table(table_middle) + split_table(table_odd)


def stream_tables(length):
    quarter = length // 4
    index = np.arange(quarter)
    angle = 2.0 * np.pi * ((index[:, None] * index[None, :]) % quarter) / quarter
    cosine, sine = np.cos(angle), np.sin(angle)
    twist = 2.0 * np.pi * (np.arange(4)[:, None] * index[None, :]) / length
    twiddle = np.concatenate((np.cos(twist), np.sin(twist)), 0).astype(np.float32)
    return split_table(np.block([[cosine, -sine], [sine, cosine]])) + (twiddle,)


def split_value(value):
    high = value.astype(jnp.bfloat16)
    low = (value - high.astype(jnp.float32)).astype(jnp.bfloat16)
    return high, low


def three_dots(left, right, dims):
    def one(a, b):
        return lax.dot_general(a, b, (dims, ((), ())), preferred_element_type=jnp.float32)

    return one(left[0], right[0]) + (one(left[1], right[0]) + one(left[0], right[1]))


NT = ((1,), (1,))
NN = ((1,), (0,))


def emit_rows(share, real, imag, out_ref):
    lane = lax.broadcasted_iota(jnp.int32, (real.shape[0], 128), 1)
    third = jnp.where(lane < 64, real[:, 128:], imag[:, 128:])
    out_ref[:, :share] = real[:, :128].reshape(-1, share, 128)
    out_ref[:, share : 2 * share] = imag[:, :128].reshape(-1, share, 128)
    out_ref[:, 2 * share :] = third.reshape(-1, share, 128)


def span_quarters(v_ref, strips):
    rows = v_ref.shape[0] // strips
    first = rows // 3 * 2

    def strip(j):
        values = v_ref[pl.ds(j, rows, stride=strips), :]
        return jnp.concatenate((values, values[first:]), 0)

    per = strips // 4
    return [
        jnp.concatenate([strip(i * per + n) for n in range(per)], 1) for i in range(4)
    ]


def span_odd(share, part, o_h, o_l, out_ref):
    quarter = part[0].shape[1]
    odd_in = jnp.concatenate((part[0] - part[2], part[1] - part[3]), 1)
    odd = three_dots((o_h[...], o_l[...]), split_value(odd_in), NT)
    emit_rows(share, odd[:quarter], odd[quarter:], out_ref)


def span_even(share, part, e_h, e_l, m_h, m_l, out_ref):
    eighth = part[0].shape[1] // 2
    plus_even, plus_odd = part[0] + part[2], part[1] + part[3]
    even = three_dots((e_h[...], e_l[...]), split_value(plus_even + plus_odd), NT)
    middle = three_dots((m_h[...], m_l[...]), split_value(plus_even - plus_odd), NT)
    real = jnp.concatenate((even[:eighth], middle[:eighth]), 0)
    imag = jnp.concatenate((even[eighth:], middle[eighth:]), 0)
    emit_rows(share, real, imag, out_ref)


def stream_stage(share, planes, owns_mean, sign, band_ref, in_ref, t_h, t_l, w_ref, cells, out_ref, send_part):
    px_count = in_ref.shape[0] // planes
    columns = px_count // 2
    group_cols = columns // 4
    quarter = w_ref.shape[1]
    lane = lax.broadcasted_iota(jnp.int32, (3 * share, 128), 1)
    low_half = lane < 64
    blocks = []
    for q in range(columns):
        real, imag = [[], [], []], [[], [], []]
        for y in range(planes):
            a = in_ref[2 * q * planes + y]
            b = in_ref[(2 * q + 1) * planes + y]
            low = jnp.where(low_half, a, pltpu.roll(b, 64, 1))
            high = jnp.where(low_half, pltpu.roll(a, 64, 1), b)
            real[0].append(low[:share])
            imag[0].append(low[share : 2 * share])
            real[1].append(high[:share])
            imag[1].append(high[share : 2 * share])
            real[2].append(low[2 * share :])
            imag[2].append(high[2 * share :])
        blocks.append(
            (
                jnp.concatenate(real[0] + real[1] + real[2], 0),
                jnp.concatenate(imag[0] + imag[1] + imag[2], 0),
            )
        )
    part = [
        tuple(
            jnp.concatenate([blocks[j * group_cols + g][ri] for g in range(group_cols)], 1)
            for ri in range(2)
        )
        for j in range(4)
    ]
    sum02 = [part[0][i] + part[2][i] for i in range(2)]
    dif02 = [part[0][i] - part[2][i] for i in range(2)]
    sum13 = [part[1][i] + part[3][i] for i in range(2)]
    dif13 = [part[1][i] - part[3][i] for i in range(2)]
    mixed = [
        (sum02[0] + sum13[0], sum02[1] + sum13[1]),
        (dif02[0] + dif13[1], dif02[1] - dif13[0]),
        (sum02[0] - sum13[0], sum02[1] - sum13[1]),
        (dif02[0] - dif13[1], dif02[1] + dif13[0]),
    ]
    turned = []
    for k1, (real, imag) in enumerate(mixed):
        if k1:
            cosine, sine = w_ref[k1 : k1 + 1], w_ref[4 + k1 : 5 + k1]
            real, imag = real * cosine + imag * sine, imag * cosine - real * sine
        turned.append(jnp.concatenate((real, imag), 1))
    table = (t_h[...], t_l[...])
    front = three_dots(split_value(jnp.concatenate(turned, 0)), table, NN)
    if owns_mean is not None:
        block = 3 * planes * share
        row = lax.broadcasted_iota(jnp.int32, (block, 2 * quarter), 0)
        col = lax.broadcasted_iota(jnp.int32, (block, 2 * quarter), 1)
        anchor = jnp.logical_and(row % share == 0, col % quarter == 0)
        anchor = jnp.logical_and(anchor, owns_mean)
        front = jnp.concatenate((jnp.where(anchor, 0.0, front[:block]), front[block:]), 0)
    front = front.reshape(4, 3, planes, share, 2 * quarter)
    tall = (4 * share, quarter)

    def spectrum(c, y, ri):
        return front[:, c, y, :, ri * quarter : (ri + 1) * quarter].reshape(tall)

    in_order = jnp.full(tall, band_ref[0], jnp.int32) == 0
    field = [
        [
            tuple(
                jnp.where(in_order, spectrum(c, b, ri), spectrum(c, 1 - b, ri)) for ri in range(2)
            )
            for b in range(NB)
        ]
        for c in range(3)
    ]
    scale = 2.0 / (cells * math.sqrt(cells))
    if owns_mean is not None:
        row = lax.broadcasted_iota(jnp.int32, tall, 0)
        single = jnp.logical_and(row % share == 0, owns_mean)
        scale = jnp.where(single, 0.5 * scale, scale)

    def banded(left, right, b):
        lr, li = field[left][b]
        rr, ri = field[right][b]
        real = (lr * rr + li * ri) * scale
        if left == right:
            return real
        return jnp.concatenate((real, (lr * ri - li * rr) * scale), 1)

    own_table = (t_h[:, :quarter], t_l[:, :quarter])

    def lines_of(members):
        value = [banded(*PAIR_LIST[m // NB], m % NB) for m in members]
        result = [None] * len(members)
        for columns_in, used in ((quarter, own_table), (2 * quarter, table)):
            chosen = [n for n in range(len(members)) if value[n].shape[1] == columns_in]
            if not chosen:
                continue
            joined = jnp.concatenate([value[n] for n in chosen], 0)
            whole = three_dots(split_value(joined), used, NT)
            for place, n in enumerate(chosen):
                result[n] = spread(whole[place * 4 * share : (place + 1) * 4 * share])
        return result

    def spread(back):
        turned = []
        for k1 in range(4):
            real = back[k1 * share : (k1 + 1) * share, :quarter]
            imag = back[k1 * share : (k1 + 1) * share, quarter:]
            if k1:
                cosine, sine = w_ref[k1 : k1 + 1], w_ref[4 + k1 : 5 + k1]
                if sign is not None and k1 % 2:
                    cosine, sine = cosine * sign, sine * sign
                real, imag = real * cosine - imag * sine, imag * cosine + real * sine
            turned.append((real, imag))
        s02 = [turned[0][i] + turned[2][i] for i in range(2)]
        d02 = [turned[0][i] - turned[2][i] for i in range(2)]
        s13 = [turned[1][i] + turned[3][i] for i in range(2)]
        d13 = [turned[1][i] - turned[3][i] for i in range(2)]
        real = [s02[0] + s13[0], d02[0] - d13[1]]
        imag = [s02[1] + s13[1], d02[1] + d13[0]]
        if sign is None:
            real += [s02[0] - s13[0], d02[0] + d13[1]]
            imag += [s02[1] - s13[1], d02[1] - d13[0]]
        return real, imag

    held = 4 * quarter if sign is None else 2 * quarter
    width = held // out_ref.shape[1]
    groups = 128 // width
    per_group = out_ref.shape[0]
    lane = lax.broadcasted_iota(jnp.int32, (share, 128), 1)
    for i in range(per_group):
        lines = lines_of([g * per_group + i for g in range(groups)])
        for ri in range(2):
            at = ri * share
            for q in range(held // 128):
                j, inside = q * 128 // quarter, q * 128 % quarter
                tiles = [lines[g][ri][j][:, inside : inside + 128] for g in range(groups)]
                for t in range(groups):
                    packed = None
                    for g in range(groups):
                        shift = (g - t) * width % 128
                        tile = pltpu.roll(tiles[g], shift, 1) if shift else tiles[g]
                        packed = tile if g == 0 else jnp.where(lane >= g * width, tile, packed)
                    out_ref[i, q * groups + t, at : at + share] = packed
        send_part(i)


def back_even(share, i, in_ref, e_h, e_l, m_h, m_l, held_ref):
    devices = in_ref.shape[1]
    eighth = devices * share // 2
    real = in_ref[i, :, :share].reshape(devices * share, 128).T
    imag = in_ref[i, :, share : 2 * share].reshape(devices * share, 128).T

    def both(start, stop):
        return split_value(jnp.concatenate((real[:, start:stop], imag[:, start:stop]), 1))

    even = three_dots(both(0, eighth), (e_h[...], e_l[...]), NN)
    middle = three_dots(both(eighth, 2 * eighth), (m_h[...], m_l[...]), NN)
    held_ref[i, 0] = even + middle
    held_ref[i, 1] = even - middle


def back_odd(share, i, in_ref, o_h, o_l, held_ref, out_ref):
    devices = in_ref.shape[1]
    groups, _, width, length = out_ref.shape
    quarter = length // 4
    real = in_ref[i, :, :share].reshape(devices * share, 128).T
    imag = in_ref[i, :, share : 2 * share].reshape(devices * share, 128).T
    odd = three_dots(split_value(jnp.concatenate((real, imag), 1)), (o_h[...], o_l[...]), NN)
    plus, minus = held_ref[i, 0], held_ref[i, 1]
    first, second = odd[:, :quarter], odd[:, quarter:]
    for j, line in enumerate((plus + first, minus + second, plus - first, minus - second)):
        out_ref[:, i, :, j * quarter : (j + 1) * quarter] = line.reshape(groups, width, quarter)


def flip_bits(index, bits):
    moved, bit = index, 1
    while bit <= bits:
        if bits & bit:
            moved = moved + bit * (1 - 2 * ((index // bit) % 2))
        bit *= 2
    return moved


def whole_kernel(
    px_count,
    py_count,
    band_ref,
    v_far,
    table_far,
    w_ref,
    out_ref,
    v_ref,
    tables,
    odd_out,
    odd_in,
    even_out,
    even_in,
    odd_back_out,
    odd_back_in,
    even_back_out,
    even_back_in,
    held,
    send_sem,
    recv_sem,
    own_sem,
    load_sem,
):
    quarter = tables.shape[1] // 2
    cuts = (0, 4 * quarter, 6 * quarter, 10 * quarter)
    loads = [pltpu.make_async_copy(v_far, v_ref, load_sem.at[0])] + [
        pltpu.make_async_copy(table_far.at[start:stop], tables.at[start:stop], load_sem.at[1 + n])
        for n, (start, stop) in enumerate(zip(cuts[:-1], cuts[1:]))
    ]
    o_h, o_l = tables.at[: 2 * quarter], tables.at[2 * quarter : 4 * quarter]
    e_h, m_h = (tables.at[4 * quarter : 5 * quarter, at : at + quarter] for at in (0, quarter))
    e_l, m_l = (tables.at[5 * quarter : 6 * quarter, at : at + quarter] for at in (0, quarter))
    t_h, t_l = tables.at[6 * quarter : 8 * quarter], tables.at[8 * quarter :]
    for load in loads:
        load.start()
    px, py = lax.axis_index("px"), lax.axis_index("py")
    count = px_count * py_count
    half = count // 2
    me = px * py_count + py
    my_owner = me % half
    parts = odd_back_out.shape[0]
    barrier = pltpu.get_barrier_semaphore()
    near, far = list(range(1, half)), list(range(half, count))
    peers = {
        s: (flip_bits(px, s // py_count), flip_bits(py, s % py_count)) for s in near + far
    }
    place = {s: peers[s][0] * py_count + peers[s][1] for s in peers}
    for s in far + near:
        pl.semaphore_signal(
            barrier, inc=1, device_id=peers[s], device_id_type=pl.DeviceIdType.MESH
        )
    moves = []

    def swap(steps, source_at, target, own_source):
        lane = len(moves)
        copies = []
        for s in steps:
            copy = pltpu.make_async_remote_copy(
                src_ref=source_at(s),
                dst_ref=target,
                send_sem=send_sem.at[lane, s],
                recv_sem=recv_sem.at[lane, s],
                device_id=peers[s],
                device_id_type=pl.DeviceIdType.MESH,
            )
            copy.start()
            copies.append(copy)
        own = pltpu.make_async_copy(own_source, target, own_sem.at[lane])
        own.start()
        moves.append((own, copies))

    def arrive(move):
        move[0].wait()
        for copy in move[1]:
            copy.wait_recv()

    odd_share, even_share = quarter // count, quarter // half
    loads[0].wait()
    loads[1].wait()
    part = span_quarters(v_ref, 4 * quarter // 128)
    span_odd(odd_share, part, o_h, o_l, odd_out)
    pl.semaphore_wait(barrier, count - 1)
    swap(far + near, lambda s: odd_out.at[place[s]], odd_in.at[me], odd_out.at[me])
    loads[2].wait()
    span_even(even_share, part, e_h, e_l, m_h, m_l, even_out)
    swap(far + near, lambda s: even_out.at[place[s] % half], even_in.at[me], even_out.at[my_owner])
    loads[3].wait()
    cells = float(4 * quarter * 4 * w_ref.shape[1])

    def send_odd(i):
        source, target = odd_back_out.at[i], odd_back_in.at[i]
        swap(far + near, lambda s: source.at[place[s]], target.at[me], source.at[me])

    def send_even(i):
        source, target = even_back_out.at[i], even_back_in.at[i]
        swap(near, lambda s: source.at[place[s] % half], target.at[my_owner], source.at[my_owner])

    arrive(moves[0])
    stream_stage(
        odd_share, py_count, None, None, band_ref, odd_in, t_h, t_l, w_ref, cells,
        odd_back_out, send_odd,
    )
    sign = (1 - 2 * (me // half)).astype(jnp.float32)
    arrive(moves[1])
    stream_stage(
        even_share, py_count, my_owner == 0, sign, band_ref, even_in, t_h, t_l, w_ref, cells,
        even_back_out, send_even,
    )
    for i in range(parts):
        arrive(moves[2 + parts + i])
        back_even(even_share, i, even_back_in, e_h, e_l, m_h, m_l, held)
    for i in range(parts):
        arrive(moves[2 + i])
        back_odd(odd_share, i, odd_back_in, o_h, o_l, held, out_ref)
    for _, copies in moves:
        for copy in copies:
            copy.wait_send()


def register_device(velocity, band_of):
    px_count = lax.axis_size("px")
    py_count = lax.axis_size("py")
    count = px_count * py_count
    _, rows_x, _, span = velocity.shape
    stream = rows_x * px_count
    half, quarter = count // 2, span // 4
    odd_share, even_share = quarter // count, quarter // half
    width = stream // count
    groups = 128 // width
    parts = len(PAIR_LIST) * NB // groups
    vmem = pl.BlockSpec(memory_space=pltpu.VMEM)
    smem = pl.BlockSpec(memory_space=pltpu.SMEM)
    far = pl.BlockSpec(memory_space=pl.ANY)
    e_h, e_l, m_h, m_l, o_h, o_l = span_tables(span)
    t_h, t_l, twiddle = stream_tables(stream)
    even = [np.concatenate(pair, 1) for pair in ((e_h, m_h), (e_l, m_l))]
    tables = np.concatenate([o_h, o_l] + even + [t_h, t_l], 0)
    strips = velocity.size // 128
    odd_shape, even_shape = (3 * odd_share, 128), (3 * even_share, 128)
    odd_back = (parts, count, 2 * odd_share, 128)
    even_back = (parts, half, 2 * even_share, 128)
    out = pl.pallas_call(
        functools.partial(whole_kernel, px_count, py_count),
        out_shape=jax.ShapeDtypeStruct((groups, parts, width, span), jnp.float32),
        in_specs=[smem, far, far, vmem],
        out_specs=vmem,
        scratch_shapes=[
            pltpu.VMEM((strips, 128), jnp.float32),
            pltpu.VMEM(tables.shape, tables.dtype),
            pltpu.VMEM((count,) + odd_shape, jnp.float32),
            pltpu.VMEM((count,) + odd_shape, jnp.float32),
            pltpu.VMEM((half,) + even_shape, jnp.float32),
            pltpu.VMEM((count,) + even_shape, jnp.float32),
            pltpu.VMEM(odd_back, jnp.float32),
            pltpu.VMEM(odd_back, jnp.float32),
            pltpu.VMEM(even_back, jnp.float32),
            pltpu.VMEM(even_back, jnp.float32),
            pltpu.VMEM((parts, 2, 128, quarter), jnp.float32),
            pltpu.SemaphoreType.DMA((2 + 2 * parts, count)),
            pltpu.SemaphoreType.DMA((2 + 2 * parts, count)),
            pltpu.SemaphoreType.DMA((2 + 2 * parts,)),
            pltpu.SemaphoreType.DMA((4,)),
        ],
        compiler_params=pltpu.CompilerParams(
            collective_id=0, has_side_effects=True, vmem_limit_bytes=64487424
        ),
    )(band_of, velocity.reshape(strips, 128), tables, twiddle)
    return out.reshape(len(PAIR_LIST), NB, width, span)


def fills_registers(velocity, px_count, py_count):
    comps, rows_x, planes, span = velocity.shape
    count = px_count * py_count
    stream = rows_x * px_count
    share = span // 2 // count
    width = max(stream // count, 1)
    return (
        comps == 3
        and rows_x == 64
        and planes == 1
        and px_count & (px_count - 1) == 0
        and py_count & (py_count - 1) == 0
        and px_count % 8 == 0
        and span % 1024 == 0
        and stream == span
        and stream == width * count
        and planes * py_count == NB
        and NB == 2
        and span == 2 * share * count
        and share % 16 == 0
        and 128 % width == 0
        and len(PAIR_LIST) * NB * width % 128 == 0
    )


def per_device(velocity, band_of):
    if fills_registers(velocity, lax.axis_size("px"), lax.axis_size("py")):
        return register_device(velocity, band_of)
    return general_device(velocity, band_of)


def solution(mesh):
    in_specs = (P(None, "px", "py", None), P())
    out_specs = P(None, None, ("px", "py"), None)
    return jax.shard_map(
        per_device, mesh=mesh, in_specs=in_specs, out_specs=out_specs, check_vma=False
    )
```

```python
import functools
import math

import jax
import jax.numpy as jnp
import numpy as np
from jax import lax
from jax.experimental import pallas as pl
from jax.experimental.pallas import tpu as pltpu
from jax.sharding import PartitionSpec as P

NB = 2


PAIR_LIST = ((0, 0), (0, 1), (0, 2), (1, 1), (1, 2), (2, 2))


def phase_table(row_values, offset, count, length):
    col_values = offset + lax.iota(jnp.int32, count)
    phase = row_values[:, None] * col_values[None, :] % length
    angle = phase.astype(jnp.float32) * (2.0 * math.pi / length)
    return (jnp.cos(angle), jnp.sin(angle))


def transform_last(real_part, imag_part, sign):
    full_shape = real_part.shape
    length = full_shape[-1]
    stacked = jnp.concatenate((real_part.reshape(-1, length), imag_part.reshape(-1, length)), 0)
    row_count = stacked.shape[0] // 2
    row_values = lax.iota(jnp.int32, length)

    def one_block(block_index, outputs):
        offset = (block_index * 128).astype(jnp.int32)
        cosine_table, sine_table = phase_table(row_values, offset, 128, length)
        with_cos = jnp.dot(
            stacked,
            cosine_table,
            precision=lax.Precision.HIGHEST,
            preferred_element_type=jnp.float32,
        )
        with_sin = jnp.dot(
            stacked, sine_table, precision=lax.Precision.HIGHEST, preferred_element_type=jnp.float32
        )
        new_real = with_cos[:row_count] - sign * with_sin[row_count:]
        new_imag = with_cos[row_count:] + sign * with_sin[:row_count]
        return (
            lax.dynamic_update_slice_in_dim(outputs[0], new_real, offset, 1),
            lax.dynamic_update_slice_in_dim(outputs[1], new_imag, offset, 1),
        )

    zeros = jnp.zeros((row_count, length), jnp.float32)
    out_real, out_imag = lax.fori_loop(0, length // 128, one_block, (zeros, zeros))
    return (out_real.reshape(full_shape), out_imag.reshape(full_shape))


def span_forward(velocity):
    comps, rows_x, planes, length = velocity.shape
    half = length // 2
    row_values = lax.iota(jnp.int32, length)

    def one_block(block_index, outputs):
        offset = (block_index * 128).astype(jnp.int32)
        cosine_table, sine_table = phase_table(row_values, offset, 128, length)
        with_cos = jnp.einsum(
            "cxpz,zk->cpkx",
            velocity,
            cosine_table,
            precision=lax.Precision.HIGHEST,
            preferred_element_type=jnp.float32,
        )
        with_sin = jnp.einsum(
            "cxpz,zk->cpkx",
            velocity,
            sine_table,
            precision=lax.Precision.HIGHEST,
            preferred_element_type=jnp.float32,
        )
        return (
            lax.dynamic_update_slice_in_dim(outputs[0], with_cos, offset, 2),
            lax.dynamic_update_slice_in_dim(outputs[1], -with_sin, offset, 2),
        )

    zeros = jnp.zeros((comps, planes, half, rows_x), jnp.float32)
    return lax.fori_loop(0, half // 128, one_block, (zeros, zeros))


def span_inverse(summed, kz_order):
    half = summed.shape[3]
    length = 2 * half
    multiplier = jnp.where(kz_order == 0, 1.0, 2.0).astype(jnp.float32)
    held_real = summed[:, :, 0] * multiplier[:, None]
    held_imag = summed[:, :, 1] * multiplier[:, None]

    def one_block(block_index, output):
        offset = (block_index * 128).astype(jnp.int32)
        cosine_table, sine_table = phase_table(kz_order, offset, 128, length)
        part = jnp.einsum(
            "sbkd,kz->sbdz",
            held_real,
            cosine_table,
            precision=lax.Precision.HIGHEST,
            preferred_element_type=jnp.float32,
        )
        part = part - jnp.einsum(
            "sbkd,kz->sbdz",
            held_imag,
            sine_table,
            precision=lax.Precision.HIGHEST,
            preferred_element_type=jnp.float32,
        )
        return lax.dynamic_update_slice_in_dim(output, part, offset, 3)

    zeros = jnp.zeros((summed.shape[0], summed.shape[1], summed.shape[4], length), jnp.float32)
    return lax.fori_loop(0, length // 128, one_block, zeros)


def general_device(velocity, band_of):
    px_count = lax.axis_size("px")
    py_count = lax.axis_size("py")
    comps, rows_x, planes, span = velocity.shape
    stream = rows_x * px_count
    half = span // 2
    local_k = half // px_count
    span_real, span_imag = span_forward(velocity)
    planes_spec = jnp.stack((span_real, span_imag), 1)
    kz_index = lax.iota(jnp.int32, local_k)
    kx_index = lax.iota(jnp.int32, stream)
    at_anchor = jnp.logical_and(
        lax.axis_index("px") == 0, jnp.logical_and(kz_index[:, None] == 0, kx_index[None, :] == 0)
    )
    keep_mask = 1.0 - at_anchor.astype(jnp.float32)
    received = lax.all_to_all(planes_spec, "px", split_axis=3, concat_axis=4, tiled=True)
    front_real, front_imag = transform_last(received[:, 0], received[:, 1], -1.0)
    spectrum = jnp.stack((front_real * keep_mask, front_imag * keep_mask), 1)
    cross_list = []
    for left_comp, right_comp in PAIR_LIST:
        left_real, left_imag = (spectrum[left_comp, 0], spectrum[left_comp, 1])
        right_real, right_imag = (spectrum[right_comp, 0], spectrum[right_comp, 1])
        cross_list.append(
            jnp.stack(
                (
                    left_real * right_real + left_imag * right_imag,
                    left_real * right_imag - left_imag * right_real,
                ),
                0,
            )
        )
    cross = jnp.stack(cross_list, 0)
    band_ids = lax.iota(jnp.int32, NB)
    onehot_all = (band_of[:, None] == band_ids[None, :]).astype(jnp.float32)
    counts = jnp.sum(onehot_all, 0)
    cells = float(stream * span)
    plane_start = lax.axis_index("py") * planes
    local_hot = lax.dynamic_slice_in_dim(onehot_all, plane_start, planes, 0)
    band_weight = local_hot / (counts[None, :] * (cells * math.sqrt(cells)))
    banded = jnp.einsum("sapkx,pb->sbakx", cross, band_weight, precision=lax.Precision.HIGHEST)
    summed = lax.psum_scatter(banded, "py", scatter_dimension=3, tiled=True)
    back_real, back_imag = transform_last(summed[:, :, 0], summed[:, :, 1], 1.0)
    exchanged = lax.all_to_all(
        lax.all_to_all(
            jnp.stack((back_real, back_imag), 2), "px", split_axis=4, concat_axis=3, tiled=True
        ),
        "py",
        split_axis=4,
        concat_axis=3,
        tiled=True,
    )
    quarter = local_k // py_count
    position = lax.iota(jnp.int32, half)
    outer = position // (px_count * quarter)
    remain = position % (px_count * quarter)
    kz_order = remain // quarter * local_k + outer * quarter + remain % quarter
    return span_inverse(exchanged, kz_order)


def split_table(table):
    high = table.astype(jnp.bfloat16)
    low = (table - high.astype(np.float64)).astype(jnp.bfloat16)
    return high, low


def span_tables(length):
    quarter, eighth = length // 4, length // 8
    column = np.arange(quarter)

    def angle(first, count):
        wave = 4 * np.arange(count) + first
        return 2.0 * np.pi * ((wave[:, None] * column[None, :]) % length) / length

    even = angle(0, eighth)
    middle = angle(2, eighth)
    odd = angle(1, quarter)
    table_even = np.concatenate((np.cos(even), -np.sin(even)), 0)
    table_middle = np.concatenate((np.cos(middle), -np.sin(middle)), 0)
    table_odd = np.block([[np.cos(odd), -np.sin(odd)], [-np.sin(odd), -np.cos(odd)]])
    return split_table(table_even) + split_table(table_middle) + split_table(table_odd)


def stream_tables(length):
    quarter = length // 4
    index = np.arange(quarter)
    angle = 2.0 * np.pi * ((index[:, None] * index[None, :]) % quarter) / quarter
    cosine, sine = np.cos(angle), np.sin(angle)
    twist = 2.0 * np.pi * (np.arange(4)[:, None] * index[None, :]) / length
    twiddle = np.concatenate((np.cos(twist), np.sin(twist)), 0).astype(np.float32)
    return split_table(np.block([[cosine, -sine], [sine, cosine]])) + (twiddle,)


def split_value(value):
    high = value.astype(jnp.bfloat16)
    low = (value - high.astype(jnp.float32)).astype(jnp.bfloat16)
    return high, low


def one_dot(left, right, dims):
    return lax.dot_general(left, right, (dims, ((), ())), preferred_element_type=jnp.float32)


NT = ((1,), (1,))
NN = ((1,), (0,))


def rows_by_table(value, table):
    high, low = split_value(value)
    rows = value.shape[0]
    by_high = one_dot(jnp.concatenate((high, low), 0), table[0], NN)
    return by_high[:rows] + (by_high[rows:] + one_dot(high, table[1], NN))


def table_by_rows(table, value):
    high, low = split_value(value)
    return one_dot(table[0], high, NT) + (
        one_dot(table[1], high, NT) + one_dot(table[0], low, NT)
    )


def span_quarters(v_ref, strips):
    rows = v_ref.shape[0] // strips
    first = rows // 3 * 2

    def strip(j):
        values = v_ref[pl.ds(j, rows, stride=strips), :]
        return jnp.concatenate((values, values[first:]), 0)

    per = strips // 4
    return [
        jnp.concatenate([strip(i * per + n) for n in range(per)], 1) for i in range(4)
    ]


def span_chunk(kind, share, part, table, out_ref):
    if kind == "odd":
        value = jnp.concatenate((part[0] - part[2], part[1] - part[3]), 1)
    else:
        ahead, behind = part[0] + part[2], part[1] + part[3]
        value = ahead + behind if kind == "even" else ahead - behind
    both = table_by_rows((table[0][...], table[1][...]), value)
    count = both.shape[0] // 2
    real, imag = both[:count], both[count:]
    lane = lax.broadcasted_iota(jnp.int32, (count, 128), 1)
    third = jnp.where(lane < 64, real[:, 128:], imag[:, 128:])
    out_ref[:, :share] = real[:, :128].reshape(-1, share, 128)
    out_ref[:, share : 2 * share] = imag[:, :128].reshape(-1, share, 128)
    out_ref[:, 2 * share :] = third.reshape(-1, share, 128)


def lane_exchange(tiles, width):
    tiles = list(tiles)
    lane = lax.broadcasted_iota(jnp.int32, tiles[0].shape, 1)
    step, size = len(tiles) // 2, 64
    while step:
        mask = lane // size % 2 == 0
        for g in range(len(tiles)):
            if g & step == 0:
                a, b = tiles[g], tiles[g + step]
                tiles[g] = jnp.where(mask, a, pltpu.roll(b, size, 1))
                tiles[g + step] = jnp.where(mask, pltpu.roll(a, 128 - size, 1), b)
        step, size = step // 2, size // 2
    return tiles


def stream_stage(share, planes, owns_mean, sign, band_ref, in_ref, t_h, t_l, w_ref, cells, out_ref, send_part):
    px_count = in_ref.shape[0] // planes
    columns = px_count // 2
    group_cols = columns // 4
    quarter = w_ref.shape[1]
    lane = lax.broadcasted_iota(jnp.int32, (3 * share, 128), 1)
    low_half = lane < 64
    blocks = []
    for q in range(columns):
        real, imag = [[], [], []], [[], [], []]
        for y in range(planes):
            a = in_ref[2 * q * planes + y]
            b = in_ref[(2 * q + 1) * planes + y]
            low = jnp.where(low_half, a, pltpu.roll(b, 64, 1))
            high = jnp.where(low_half, pltpu.roll(a, 64, 1), b)
            real[0].append(low[:share])
            imag[0].append(low[share : 2 * share])
            real[1].append(high[:share])
            imag[1].append(high[share : 2 * share])
            real[2].append(low[2 * share :])
            imag[2].append(high[2 * share :])
        blocks.append(
            (
                jnp.concatenate(real[0] + real[1] + real[2], 0),
                jnp.concatenate(imag[0] + imag[1] + imag[2], 0),
            )
        )
    part = [
        tuple(
            jnp.concatenate([blocks[j * group_cols + g][ri] for g in range(group_cols)], 1)
            for ri in range(2)
        )
        for j in range(4)
    ]

    def cross4(v):
        s02 = [v[0][i] + v[2][i] for i in range(2)]
        d02 = [v[0][i] - v[2][i] for i in range(2)]
        s13 = [v[1][i] + v[3][i] for i in range(2)]
        d13 = [v[1][i] - v[3][i] for i in range(2)]
        return [
            (s02[0] + s13[0], s02[1] + s13[1]),
            (d02[0] + d13[1], d02[1] - d13[0]),
            (s02[0] - s13[0], s02[1] - s13[1]),
            (d02[0] - d13[1], d02[1] + d13[0]),
        ]

    turned = []
    for k1, (real, imag) in enumerate(cross4(part)):
        if k1:
            cosine, sine = w_ref[k1 : k1 + 1], w_ref[4 + k1 : 5 + k1]
            real, imag = real * cosine + imag * sine, imag * cosine - real * sine
        turned.append(jnp.concatenate((real, imag), 1))
    table = (t_h[...], t_l[...])
    front = rows_by_table(jnp.concatenate(turned, 0), table)
    if owns_mean is not None:
        block = 3 * planes * share
        row = lax.broadcasted_iota(jnp.int32, (block, 2 * quarter), 0)
        col = lax.broadcasted_iota(jnp.int32, (block, 2 * quarter), 1)
        anchor = jnp.logical_and(row % share == 0, col % quarter == 0)
        anchor = jnp.logical_and(anchor, owns_mean)
        front = jnp.concatenate((jnp.where(anchor, 0.0, front[:block]), front[block:]), 0)
    front = front.reshape(4, 3, planes, share, 2 * quarter)
    tall = (4 * share, quarter)

    def spectrum(c, y, ri):
        return front[:, c, y, :, ri * quarter : (ri + 1) * quarter].reshape(tall)

    in_order = jnp.full(tall, band_ref[0], jnp.int32) == 0
    field = [
        [
            tuple(
                jnp.where(in_order, spectrum(c, b, ri), spectrum(c, 1 - b, ri)) for ri in range(2)
            )
            for b in range(NB)
        ]
        for c in range(3)
    ]
    scale = 2.0 / (cells * math.sqrt(cells))
    if owns_mean is not None:
        row = lax.broadcasted_iota(jnp.int32, tall, 0)
        single = jnp.logical_and(row % share == 0, owns_mean)
        scale = jnp.where(single, 0.5 * scale, scale)

    def banded(left, right, b):
        lr, li = field[left][b]
        rr, ri = field[right][b]
        real = (lr * rr + li * ri) * scale
        if left == right:
            return real
        return jnp.concatenate((real, (li * rr - lr * ri) * scale), 1)

    members = list(range(len(PAIR_LIST) * NB))
    lines = [None] * len(members)
    own_table = (t_h[:quarter], t_l[:quarter])
    for alike, used in ((True, own_table), (False, table)):
        chosen = [m for m in members if (len(set(PAIR_LIST[m // NB])) == 1) == alike]
        joined = jnp.concatenate([banded(*PAIR_LIST[m // NB], m % NB) for m in chosen], 0)
        whole = rows_by_table(joined, used)
        for at, m in enumerate(chosen):
            back = whole[at * 4 * share : (at + 1) * 4 * share]
            turned = []
            for k1 in range(4):
                real = back[k1 * share : (k1 + 1) * share, :quarter]
                imag = back[k1 * share : (k1 + 1) * share, quarter:]
                if k1:
                    cosine, sine = w_ref[k1 : k1 + 1], w_ref[4 + k1 : 5 + k1]
                    if sign is not None and k1 % 2:
                        cosine, sine = cosine * sign, sine * sign
                    real, imag = real * cosine + imag * sine, imag * cosine - real * sine
                turned.append((real, imag))
            lines[m] = cross4(turned)
    held = 4 * quarter if sign is None else 2 * quarter
    width = held // out_ref.shape[0]
    groups = 128 // width
    per_group = len(members) // groups
    for i in range(per_group):
        for ri in range(2):
            at = (i * 2 + ri) * share
            for q in range(held // 128):
                j, inside = q * 128 // quarter, q * 128 % quarter
                tiles = [
                    lines[g * per_group + i][j][ri][:, inside : inside + 128]
                    for g in range(groups)
                ]
                for t, packed in enumerate(lane_exchange(tiles, width)):
                    out_ref[q * groups + t, at : at + share] = packed
        send_part(i)


def back_chunk(share, parts, in_ref, table, keep_ref):
    sources = in_ref.shape[0]

    def turned(i, ri):
        at = (i * 2 + ri) * share
        return in_ref[:, at : at + share].reshape(sources * share, 128).T

    value = jnp.concatenate(
        [jnp.concatenate((turned(i, 0), -turned(i, 1)), 1) for i in range(parts)], 0
    )
    keep_ref[...] = rows_by_table(value, (table[0][...], table[1][...]))


def flip_bits(index, bits):
    moved, bit = index, 1
    while bit <= bits:
        if bits & bit:
            moved = moved + bit * (1 - 2 * ((index // bit) % 2))
        bit *= 2
    return moved


ORDER = ("even", "odd", "middle")
BACK_ORDER = ("even", "middle", "odd")
SEND_ORDER = "down"


def whole_kernel(
    px_count,
    py_count,
    share,
    parts,
    band_ref,
    v_ref,
    table_far,
    w_ref,
    out_ref,
    tables,
    span_out_even,
    span_out_middle,
    span_out_odd,
    span_in,
    back_out_even,
    back_out_middle,
    back_out_odd,
    back_in_even,
    back_in_middle,
    back_in_odd,
    keep_even,
    keep_middle,
    keep_odd,
    send_sem,
    recv_sem,
    own_sem,
    load_sem,
):
    quarter = tables.shape[1] // 2
    cuts = (0, 2 * quarter, 6 * quarter, 10 * quarter)
    loads = [
        pltpu.make_async_copy(table_far.at[start:stop], tables.at[start:stop], load_sem.at[n])
        for n, (start, stop) in enumerate(zip(cuts[:-1], cuts[1:]))
    ]
    span_table = {
        "even": [tables.at[n * quarter : (n + 1) * quarter, :quarter] for n in range(2)],
        "middle": [tables.at[n * quarter : (n + 1) * quarter, quarter:] for n in range(2)],
        "odd": [tables.at[n * quarter : (n + 2) * quarter] for n in (2, 4)],
    }
    t_h, t_l = tables.at[6 * quarter : 8 * quarter], tables.at[8 * quarter :]
    for load in loads:
        load.start()
    px, py = lax.axis_index("px"), lax.axis_index("py")
    count = px_count * py_count
    half = count // 2
    me = px * py_count + py
    my_owner = me % half
    barrier = pltpu.get_barrier_semaphore()
    near, far = list(range(1, half)), list(range(half, count))
    peers = {
        s: (flip_bits(px, s // py_count), flip_bits(py, s % py_count)) for s in near + far
    }
    place = {s: peers[s][0] * py_count + peers[s][1] for s in peers}
    for s in far + near:
        pl.semaphore_signal(
            barrier, inc=1, device_id=peers[s], device_id_type=pl.DeviceIdType.MESH
        )
    moves = {}

    def swap(name, steps, source_at, target, own_source):
        lane = len(moves)
        copies = []
        for s in steps:
            copy = pltpu.make_async_remote_copy(
                src_ref=source_at(s),
                dst_ref=target,
                send_sem=send_sem.at[lane, s],
                recv_sem=recv_sem.at[lane, s],
                device_id=peers[s],
                device_id_type=pl.DeviceIdType.MESH,
            )
            copy.start()
            copies.append(copy)
        own = pltpu.make_async_copy(own_source, target, own_sem.at[lane])
        own.start()
        moves[name] = (own, copies)

    def arrive(name):
        moves[name][0].wait()
        for copy in moves[name][1]:
            copy.wait_recv()

    if SEND_ORDER == "near":
        everyone, beside = near + far, near
    elif SEND_ORDER == "far":
        everyone, beside = far + near, near
    else:
        everyone, beside = (near + far)[::-1], near[::-1]
    span_out = {"even": span_out_even, "middle": span_out_middle, "odd": span_out_odd}
    back_out = {"even": back_out_even, "middle": back_out_middle, "odd": back_out_odd}
    back_in = {"even": back_in_even, "middle": back_in_middle, "odd": back_in_odd}
    keep = {"even": keep_even, "middle": keep_middle, "odd": keep_odd}
    loads[0].wait()
    loads[1].wait()
    part = span_quarters(v_ref, 4 * quarter // 128)
    for n, kind in enumerate(ORDER):
        span_chunk(kind, share, part, span_table[kind], span_out[kind])
        if n == 0:
            pl.semaphore_wait(barrier, count - 1)
        source, owners = span_out[kind], count if kind == "odd" else half
        swap(
            kind,
            everyone,
            lambda s: source.at[place[s] % owners],
            span_in.at[n, me],
            source.at[me % owners],
        )
    loads[2].wait()
    cells = float(4 * quarter * 4 * w_ref.shape[1])
    sign = (1 - 2 * (me // half)).astype(jnp.float32)
    for n, kind in enumerate(ORDER):
        arrive(kind)
        source, target = back_out[kind], back_in[kind]

        def send(i):
            rows = slice(None)
            if kind == ORDER[-1] and False:
                rows = slice(i * 2 * share, (i + 1) * 2 * share)
            elif i < parts - 1:
                return
            if kind == "odd":
                swap(kind + "-back", everyone, lambda s: source.at[place[s], rows], target.at[me, rows], source.at[me, rows])
            else:
                swap(
                    kind + "-back" + (str(i) if kind == ORDER[-1] and False else ""),
                    beside,
                    lambda s: source.at[place[s] % half, rows],
                    target.at[my_owner, rows],
                    source.at[my_owner, rows],
                )

        stream_stage(
            share,
            py_count,
            my_owner == 0 if kind == "even" else None,
            None if kind == "odd" else sign,
            band_ref,
            span_in.at[n],
            t_h,
            t_l,
            w_ref,
            cells,
            source,
            send,
        )
    groups, _, width, _ = out_ref.shape
    done = []
    for kind in BACK_ORDER:
        for name in list(moves):
            if name.startswith(kind + "-back"):
                arrive(name)
        back_chunk(share, parts, back_in[kind], span_table[kind], keep[kind])
        done.append(kind)
        if len(done) == 1:
            continue
        for i in range(parts):
            rows = slice(i * 128, (i + 1) * 128)
            for j in range(4):
                span = slice(j * quarter, (j + 1) * quarter)
                terms = done if len(done) == 2 else done[2:]
                line = None
                for term in terms:
                    at = slice(quarter, 2 * quarter) if term == "odd" and j % 2 else slice(0, quarter)
                    value = keep[term][rows, at].reshape(groups, width, quarter)
                    minus = (term == "middle" and j % 2) or (term == "odd" and j >= 2)
                    if line is None and len(done) == 3:
                        line = out_ref[:, i, :, span]
                    if line is None:
                        line = -value if minus else value
                    else:
                        line = line - value if minus else line + value
                out_ref[:, i, :, span] = line
    for _, copies in moves.values():
        for copy in copies:
            copy.wait_send()


def register_device(velocity, band_of):
    px_count = lax.axis_size("px")
    py_count = lax.axis_size("py")
    count = px_count * py_count
    _, rows_x, _, span = velocity.shape
    stream = rows_x * px_count
    half, quarter = count // 2, span // 4
    share = quarter // count
    width = stream // count
    groups = 128 // width
    parts = len(PAIR_LIST) * NB // groups
    vmem = pl.BlockSpec(memory_space=pltpu.VMEM)
    smem = pl.BlockSpec(memory_space=pltpu.SMEM)
    far = pl.BlockSpec(memory_space=pl.ANY)
    e_h, e_l, m_h, m_l, o_h, o_l = span_tables(span)
    t_h, t_l, twiddle = stream_tables(stream)
    even = [np.concatenate(pair, 1) for pair in ((e_h, m_h), (e_l, m_l))]
    tables = np.concatenate(even + [o_h, o_l, t_h, t_l], 0)
    strips = velocity.size // 128
    rows_in, rows_back = 3 * share, 2 * parts * share
    spans = [(half, rows_in, 128), (half, rows_in, 128), (count, rows_in, 128), (3, count, rows_in, 128)]
    backs = [(n, rows_back, 128) for n in (half, half, count)]
    keeps = [(parts * 128, n * quarter) for n in (1, 1, 2)]
    lanes = 6 + parts
    out = pl.pallas_call(
        functools.partial(whole_kernel, px_count, py_count, share, parts),
        out_shape=jax.ShapeDtypeStruct((groups, parts, width, span), jnp.float32),
        in_specs=[smem, vmem, far, vmem],
        out_specs=vmem,
        scratch_shapes=[pltpu.VMEM(tables.shape, tables.dtype)]
        + [pltpu.VMEM(shape, jnp.float32) for shape in spans + backs + backs + keeps]
        + [
            pltpu.SemaphoreType.DMA((lanes, count)),
            pltpu.SemaphoreType.DMA((lanes, count)),
            pltpu.SemaphoreType.DMA((lanes,)),
            pltpu.SemaphoreType.DMA((3,)),
        ],
        compiler_params=pltpu.CompilerParams(
            collective_id=0, has_side_effects=True, vmem_limit_bytes=53000000
        ),
    )(band_of, velocity.reshape(strips, 128), tables, twiddle)
    return out.reshape(len(PAIR_LIST), NB, width, span)


def fills_registers(velocity, px_count, py_count):
    comps, rows_x, planes, span = velocity.shape
    count = px_count * py_count
    stream = rows_x * px_count
    share = span // 2 // count
    width = max(stream // count, 1)
    return (
        comps == 3
        and rows_x == 64
        and planes == 1
        and px_count & (px_count - 1) == 0
        and py_count & (py_count - 1) == 0
        and px_count % 8 == 0
        and span % 1024 == 0
        and stream == span
        and stream == width * count
        and planes * py_count == NB
        and NB == 2
        and span == 2 * share * count
        and share == 16
        and width == 32
        and 128 % width == 0
        and len(PAIR_LIST) * NB * width % 128 == 0
    )


def per_device(velocity, band_of):
    if fills_registers(velocity, lax.axis_size("px"), lax.axis_size("py")):
        return register_device(velocity, band_of)
    return general_device(velocity, band_of)


def solution(mesh):
    in_specs = (P(None, "px", "py", None), P())
    out_specs = P(None, None, ("px", "py"), None)
    return jax.shard_map(
        per_device, mesh=mesh, in_specs=in_specs, out_specs=out_specs, check_vma=False
    )
```

```python
import functools
import math

import jax
import jax.numpy as jnp
import numpy as np
from jax import lax
from jax.experimental import pallas as pl
from jax.experimental.pallas import tpu as pltpu
from jax.sharding import PartitionSpec as P

NB = 2


PAIR_LIST = ((0, 0), (0, 1), (0, 2), (1, 1), (1, 2), (2, 2))


def phase_table(row_values, offset, count, length):
    col_values = offset + lax.iota(jnp.int32, count)
    phase = row_values[:, None] * col_values[None, :] % length
    angle = phase.astype(jnp.float32) * (2.0 * math.pi / length)
    return (jnp.cos(angle), jnp.sin(angle))


def transform_last(real_part, imag_part, sign):
    full_shape = real_part.shape
    length = full_shape[-1]
    stacked = jnp.concatenate((real_part.reshape(-1, length), imag_part.reshape(-1, length)), 0)
    row_count = stacked.shape[0] // 2
    row_values = lax.iota(jnp.int32, length)

    def one_block(block_index, outputs):
        offset = (block_index * 128).astype(jnp.int32)
        cosine_table, sine_table = phase_table(row_values, offset, 128, length)
        with_cos = jnp.dot(
            stacked,
            cosine_table,
            precision=lax.Precision.HIGHEST,
            preferred_element_type=jnp.float32,
        )
        with_sin = jnp.dot(
            stacked, sine_table, precision=lax.Precision.HIGHEST, preferred_element_type=jnp.float32
        )
        new_real = with_cos[:row_count] - sign * with_sin[row_count:]
        new_imag = with_cos[row_count:] + sign * with_sin[:row_count]
        return (
            lax.dynamic_update_slice_in_dim(outputs[0], new_real, offset, 1),
            lax.dynamic_update_slice_in_dim(outputs[1], new_imag, offset, 1),
        )

    zeros = jnp.zeros((row_count, length), jnp.float32)
    out_real, out_imag = lax.fori_loop(0, length // 128, one_block, (zeros, zeros))
    return (out_real.reshape(full_shape), out_imag.reshape(full_shape))


def span_forward(velocity):
    comps, rows_x, planes, length = velocity.shape
    half = length // 2
    row_values = lax.iota(jnp.int32, length)

    def one_block(block_index, outputs):
        offset = (block_index * 128).astype(jnp.int32)
        cosine_table, sine_table = phase_table(row_values, offset, 128, length)
        with_cos = jnp.einsum(
            "cxpz,zk->cpkx",
            velocity,
            cosine_table,
            precision=lax.Precision.HIGHEST,
            preferred_element_type=jnp.float32,
        )
        with_sin = jnp.einsum(
            "cxpz,zk->cpkx",
            velocity,
            sine_table,
            precision=lax.Precision.HIGHEST,
            preferred_element_type=jnp.float32,
        )
        return (
            lax.dynamic_update_slice_in_dim(outputs[0], with_cos, offset, 2),
            lax.dynamic_update_slice_in_dim(outputs[1], -with_sin, offset, 2),
        )

    zeros = jnp.zeros((comps, planes, half, rows_x), jnp.float32)
    return lax.fori_loop(0, half // 128, one_block, (zeros, zeros))


def span_inverse(summed, kz_order):
    half = summed.shape[3]
    length = 2 * half
    multiplier = jnp.where(kz_order == 0, 1.0, 2.0).astype(jnp.float32)
    held_real = summed[:, :, 0] * multiplier[:, None]
    held_imag = summed[:, :, 1] * multiplier[:, None]

    def one_block(block_index, output):
        offset = (block_index * 128).astype(jnp.int32)
        cosine_table, sine_table = phase_table(kz_order, offset, 128, length)
        part = jnp.einsum(
            "sbkd,kz->sbdz",
            held_real,
            cosine_table,
            precision=lax.Precision.HIGHEST,
            preferred_element_type=jnp.float32,
        )
        part = part - jnp.einsum(
            "sbkd,kz->sbdz",
            held_imag,
            sine_table,
            precision=lax.Precision.HIGHEST,
            preferred_element_type=jnp.float32,
        )
        return lax.dynamic_update_slice_in_dim(output, part, offset, 3)

    zeros = jnp.zeros((summed.shape[0], summed.shape[1], summed.shape[4], length), jnp.float32)
    return lax.fori_loop(0, length // 128, one_block, zeros)


def general_device(velocity, band_of):
    px_count = lax.axis_size("px")
    py_count = lax.axis_size("py")
    comps, rows_x, planes, span = velocity.shape
    stream = rows_x * px_count
    half = span // 2
    local_k = half // px_count
    span_real, span_imag = span_forward(velocity)
    planes_spec = jnp.stack((span_real, span_imag), 1)
    kz_index = lax.iota(jnp.int32, local_k)
    kx_index = lax.iota(jnp.int32, stream)
    at_anchor = jnp.logical_and(
        lax.axis_index("px") == 0, jnp.logical_and(kz_index[:, None] == 0, kx_index[None, :] == 0)
    )
    keep_mask = 1.0 - at_anchor.astype(jnp.float32)
    received = lax.all_to_all(planes_spec, "px", split_axis=3, concat_axis=4, tiled=True)
    front_real, front_imag = transform_last(received[:, 0], received[:, 1], -1.0)
    spectrum = jnp.stack((front_real * keep_mask, front_imag * keep_mask), 1)
    cross_list = []
    for left_comp, right_comp in PAIR_LIST:
        left_real, left_imag = (spectrum[left_comp, 0], spectrum[left_comp, 1])
        right_real, right_imag = (spectrum[right_comp, 0], spectrum[right_comp, 1])
        cross_list.append(
            jnp.stack(
                (
                    left_real * right_real + left_imag * right_imag,
                    left_real * right_imag - left_imag * right_real,
                ),
                0,
            )
        )
    cross = jnp.stack(cross_list, 0)
    band_ids = lax.iota(jnp.int32, NB)
    onehot_all = (band_of[:, None] == band_ids[None, :]).astype(jnp.float32)
    counts = jnp.sum(onehot_all, 0)
    cells = float(stream * span)
    plane_start = lax.axis_index("py") * planes
    local_hot = lax.dynamic_slice_in_dim(onehot_all, plane_start, planes, 0)
    band_weight = local_hot / (counts[None, :] * (cells * math.sqrt(cells)))
    banded = jnp.einsum("sapkx,pb->sbakx", cross, band_weight, precision=lax.Precision.HIGHEST)
    summed = lax.psum_scatter(banded, "py", scatter_dimension=3, tiled=True)
    back_real, back_imag = transform_last(summed[:, :, 0], summed[:, :, 1], 1.0)
    exchanged = lax.all_to_all(
        lax.all_to_all(
            jnp.stack((back_real, back_imag), 2), "px", split_axis=4, concat_axis=3, tiled=True
        ),
        "py",
        split_axis=4,
        concat_axis=3,
        tiled=True,
    )
    quarter = local_k // py_count
    position = lax.iota(jnp.int32, half)
    outer = position // (px_count * quarter)
    remain = position % (px_count * quarter)
    kz_order = remain // quarter * local_k + outer * quarter + remain % quarter
    return span_inverse(exchanged, kz_order)


def split_table(table):
    high = table.astype(jnp.bfloat16)
    low = (table - high.astype(np.float64)).astype(jnp.bfloat16)
    return high, low


def span_tables(length):
    quarter, eighth = length // 4, length // 8
    column = np.arange(quarter)

    def angle(first, count):
        wave = 4 * np.arange(count) + first
        return 2.0 * np.pi * ((wave[:, None] * column[None, :]) % length) / length

    even = angle(0, eighth)
    middle = angle(2, eighth)
    odd = angle(1, quarter)
    table_even = np.concatenate((np.cos(even), -np.sin(even)), 0)
    table_middle = np.concatenate((np.cos(middle), -np.sin(middle)), 0)
    table_odd = np.block([[np.cos(odd), -np.sin(odd)], [-np.sin(odd), -np.cos(odd)]])
    return split_table(table_even) + split_table(table_middle) + split_table(table_odd)


def stream_tables(length):
    quarter = length // 4
    index = np.arange(quarter)
    angle = 2.0 * np.pi * ((index[:, None] * index[None, :]) % quarter) / quarter
    cosine, sine = np.cos(angle), np.sin(angle)
    twist = 2.0 * np.pi * (np.arange(4)[:, None] * index[None, :]) / length
    twiddle = np.concatenate((np.cos(twist), np.sin(twist)), 0).astype(np.float32)
    return split_table(np.block([[cosine, -sine], [sine, cosine]])) + (twiddle,)


def split_value(value):
    high = value.astype(jnp.bfloat16)
    low = (value - high.astype(jnp.float32)).astype(jnp.bfloat16)
    return high, low


def one_dot(left, right, dims):
    return lax.dot_general(left, right, (dims, ((), ())), preferred_element_type=jnp.float32)


NT = ((1,), (1,))
NN = ((1,), (0,))


def rows_by_table(value, table):
    high, low = split_value(value)
    rows = value.shape[0]
    by_high = one_dot(jnp.concatenate((high, low), 0), table[0], NN)
    return by_high[:rows] + (by_high[rows:] + one_dot(high, table[1], NN))


def table_by_rows(table, value):
    high, low = split_value(value)
    return one_dot(table[0], high, NT) + (
        one_dot(table[1], high, NT) + one_dot(table[0], low, NT)
    )


def span_quarters(v_ref, strips):
    rows = v_ref.shape[0] // strips
    first = rows // 3 * 2

    def strip(j):
        values = v_ref[pl.ds(j, rows, stride=strips), :]
        return jnp.concatenate((values, values[first:]), 0)

    per = strips // 4
    return [
        jnp.concatenate([strip(i * per + n) for n in range(per)], 1) for i in range(4)
    ]


def span_chunk(kind, share, part, table, out_ref):
    if kind == "odd":
        value = jnp.concatenate((part[0] - part[2], part[1] - part[3]), 1)
    else:
        ahead, behind = part[0] + part[2], part[1] + part[3]
        value = ahead + behind if kind == "even" else ahead - behind
    both = table_by_rows((table[0][...], table[1][...]), value)
    count = both.shape[0] // 2
    real, imag = both[:count], both[count:]
    lane = lax.broadcasted_iota(jnp.int32, (count, 128), 1)
    third = jnp.where(lane < 64, real[:, 128:], imag[:, 128:])
    out_ref[:, :share] = real[:, :128].reshape(-1, share, 128)
    out_ref[:, share : 2 * share] = imag[:, :128].reshape(-1, share, 128)
    out_ref[:, 2 * share :] = third.reshape(-1, share, 128)


def lane_exchange(tiles, width):
    tiles = list(tiles)
    lane = lax.broadcasted_iota(jnp.int32, tiles[0].shape, 1)
    step, size = len(tiles) // 2, 64
    while step:
        mask = lane // size % 2 == 0
        for g in range(len(tiles)):
            if g & step == 0:
                a, b = tiles[g], tiles[g + step]
                tiles[g] = jnp.where(mask, a, pltpu.roll(b, size, 1))
                tiles[g + step] = jnp.where(mask, pltpu.roll(a, 128 - size, 1), b)
        step, size = step // 2, size // 2
    return tiles


def stream_stage(share, planes, owns_mean, sign, band_ref, in_ref, t_h, t_l, w_ref, cells, out_ref, send_part):
    px_count = in_ref.shape[0] // planes
    columns = px_count // 2
    group_cols = columns // 4
    quarter = w_ref.shape[1]
    lane = lax.broadcasted_iota(jnp.int32, (3 * share, 128), 1)
    low_half = lane < 64
    blocks = []
    for q in range(columns):
        real, imag = [[], [], []], [[], [], []]
        for y in range(planes):
            a = in_ref[2 * q * planes + y]
            b = in_ref[(2 * q + 1) * planes + y]
            low = jnp.where(low_half, a, pltpu.roll(b, 64, 1))
            high = jnp.where(low_half, pltpu.roll(a, 64, 1), b)
            real[0].append(low[:share])
            imag[0].append(low[share : 2 * share])
            real[1].append(high[:share])
            imag[1].append(high[share : 2 * share])
            real[2].append(low[2 * share :])
            imag[2].append(high[2 * share :])
        blocks.append(
            (
                jnp.concatenate(real[0] + real[1] + real[2], 0),
                jnp.concatenate(imag[0] + imag[1] + imag[2], 0),
            )
        )
    part = [
        tuple(
            jnp.concatenate([blocks[j * group_cols + g][ri] for g in range(group_cols)], 1)
            for ri in range(2)
        )
        for j in range(4)
    ]

    def cross4(v):
        s02 = [v[0][i] + v[2][i] for i in range(2)]
        d02 = [v[0][i] - v[2][i] for i in range(2)]
        s13 = [v[1][i] + v[3][i] for i in range(2)]
        d13 = [v[1][i] - v[3][i] for i in range(2)]
        return [
            (s02[0] + s13[0], s02[1] + s13[1]),
            (d02[0] + d13[1], d02[1] - d13[0]),
            (s02[0] - s13[0], s02[1] - s13[1]),
            (d02[0] - d13[1], d02[1] + d13[0]),
        ]

    turned = []
    for k1, (real, imag) in enumerate(cross4(part)):
        if k1:
            cosine, sine = w_ref[k1 : k1 + 1], w_ref[4 + k1 : 5 + k1]
            real, imag = real * cosine + imag * sine, imag * cosine - real * sine
        turned.append(jnp.concatenate((real, imag), 1))
    table = (t_h[...], t_l[...])
    front = rows_by_table(jnp.concatenate(turned, 0), table)
    if owns_mean is not None:
        block = 3 * planes * share
        row = lax.broadcasted_iota(jnp.int32, (block, 2 * quarter), 0)
        col = lax.broadcasted_iota(jnp.int32, (block, 2 * quarter), 1)
        anchor = jnp.logical_and(row % share == 0, col % quarter == 0)
        anchor = jnp.logical_and(anchor, owns_mean)
        front = jnp.concatenate((jnp.where(anchor, 0.0, front[:block]), front[block:]), 0)
    front = front.reshape(4, 3, planes, share, 2 * quarter)
    tall = (4 * share, quarter)

    def spectrum(c, y, ri):
        return front[:, c, y, :, ri * quarter : (ri + 1) * quarter].reshape(tall)

    in_order = jnp.full(tall, band_ref[0], jnp.int32) == 0
    field = [
        [
            tuple(
                jnp.where(in_order, spectrum(c, b, ri), spectrum(c, 1 - b, ri)) for ri in range(2)
            )
            for b in range(NB)
        ]
        for c in range(3)
    ]
    scale = 2.0 / (cells * math.sqrt(cells))
    if owns_mean is not None:
        row = lax.broadcasted_iota(jnp.int32, tall, 0)
        single = jnp.logical_and(row % share == 0, owns_mean)
        scale = jnp.where(single, 0.5 * scale, scale)

    def banded(left, right, b):
        lr, li = field[left][b]
        rr, ri = field[right][b]
        real = (lr * rr + li * ri) * scale
        if left == right:
            return real
        return jnp.concatenate((real, (li * rr - lr * ri) * scale), 1)

    members = list(range(len(PAIR_LIST) * NB))
    lines = [None] * len(members)
    own_table = (t_h[:quarter], t_l[:quarter])
    for alike, used in ((True, own_table), (False, table)):
        chosen = [m for m in members if (len(set(PAIR_LIST[m // NB])) == 1) == alike]
        joined = jnp.concatenate([banded(*PAIR_LIST[m // NB], m % NB) for m in chosen], 0)
        whole = rows_by_table(joined, used)
        for at, m in enumerate(chosen):
            back = whole[at * 4 * share : (at + 1) * 4 * share]
            turned = []
            for k1 in range(4):
                real = back[k1 * share : (k1 + 1) * share, :quarter]
                imag = back[k1 * share : (k1 + 1) * share, quarter:]
                if k1:
                    cosine, sine = w_ref[k1 : k1 + 1], w_ref[4 + k1 : 5 + k1]
                    if sign is not None and k1 % 2:
                        cosine, sine = cosine * sign, sine * sign
                    real, imag = real * cosine + imag * sine, imag * cosine - real * sine
                turned.append((real, imag))
            lines[m] = cross4(turned)
    held = 4 * quarter if sign is None else 2 * quarter
    width = held // out_ref.shape[0]
    groups = 128 // width
    per_group = len(members) // groups
    for i in range(per_group):
        for ri in range(2):
            at = (i * 2 + ri) * share
            for q in range(held // 128):
                j, inside = q * 128 // quarter, q * 128 % quarter
                tiles = [
                    lines[g * per_group + i][j][ri][:, inside : inside + 128]
                    for g in range(groups)
                ]
                for t, packed in enumerate(lane_exchange(tiles, width)):
                    out_ref[q * groups + t, at : at + share] = packed
        send_part(i)


def back_chunk(share, parts, in_ref, table, keep_ref):
    sources = in_ref.shape[0]

    def turned(i, ri):
        at = (i * 2 + ri) * share
        return in_ref[:, at : at + share].reshape(sources * share, 128).T

    value = jnp.concatenate(
        [jnp.concatenate((turned(i, 0), -turned(i, 1)), 1) for i in range(parts)], 0
    )
    keep_ref[...] = rows_by_table(value, (table[0][...], table[1][...]))


def flip_bits(index, bits):
    moved, bit = index, 1
    while bit <= bits:
        if bits & bit:
            moved = moved + bit * (1 - 2 * ((index // bit) % 2))
        bit *= 2
    return moved


ORDER = ("even", "odd", "middle")
BACK_ORDER = ("even", "middle", "odd")
SEND_ORDER = "down"


def whole_kernel(
    px_count,
    py_count,
    share,
    parts,
    band_far,
    v_far,
    table_far,
    w_far,
    out_ref,
    band_ref,
    v_ref,
    w_ref,
    tables,
    span_out_even,
    span_out_middle,
    span_out_odd,
    span_in,
    back_out_even,
    back_out_middle,
    back_out_odd,
    back_in_even,
    back_in_middle,
    back_in_odd,
    keep_even,
    keep_middle,
    keep_odd,
    send_sem,
    recv_sem,
    own_sem,
    load_sem,
):
    quarter = tables.shape[1] // 2
    cuts = (0, 2 * quarter, 6 * quarter, 10 * quarter)
    pairs = [(v_far, v_ref)]
    pairs += [
        (table_far.at[start:stop], tables.at[start:stop])
        for start, stop in zip(cuts[:-1], cuts[1:])
    ]
    pairs += [(w_far, w_ref), (band_far, band_ref)]
    loads = [
        pltpu.make_async_copy(source, target, load_sem.at[n])
        for n, (source, target) in enumerate(pairs)
    ]
    span_table = {
        "even": [tables.at[n * quarter : (n + 1) * quarter, :quarter] for n in range(2)],
        "middle": [tables.at[n * quarter : (n + 1) * quarter, quarter:] for n in range(2)],
        "odd": [tables.at[n * quarter : (n + 2) * quarter] for n in (2, 4)],
    }
    t_h, t_l = tables.at[6 * quarter : 8 * quarter], tables.at[8 * quarter :]
    for load in loads:
        load.start()
    px, py = lax.axis_index("px"), lax.axis_index("py")
    count = px_count * py_count
    half = count // 2
    me = px * py_count + py
    my_owner = me % half
    barrier = pltpu.get_barrier_semaphore()
    near, far = list(range(1, half)), list(range(half, count))
    peers = {
        s: (flip_bits(px, s // py_count), flip_bits(py, s % py_count)) for s in near + far
    }
    place = {s: peers[s][0] * py_count + peers[s][1] for s in peers}
    for s in far + near:
        pl.semaphore_signal(
            barrier, inc=1, device_id=peers[s], device_id_type=pl.DeviceIdType.MESH
        )
    moves = {}

    def swap(name, steps, source_at, target, own_source):
        lane = len(moves)
        copies = []
        for s in steps:
            copy = pltpu.make_async_remote_copy(
                src_ref=source_at(s),
                dst_ref=target,
                send_sem=send_sem.at[lane, s],
                recv_sem=recv_sem.at[lane, s],
                device_id=peers[s],
                device_id_type=pl.DeviceIdType.MESH,
            )
            copy.start()
            copies.append(copy)
        own = pltpu.make_async_copy(own_source, target, own_sem.at[lane])
        own.start()
        moves[name] = (own, copies)

    def arrive(name):
        moves[name][0].wait()
        for copy in moves[name][1]:
            copy.wait_recv()

    if SEND_ORDER == "near":
        everyone, beside = near + far, near
    elif SEND_ORDER == "far":
        everyone, beside = far + near, near
    else:
        everyone, beside = (near + far)[::-1], near[::-1]
    span_out = {"even": span_out_even, "middle": span_out_middle, "odd": span_out_odd}
    back_out = {"even": back_out_even, "middle": back_out_middle, "odd": back_out_odd}
    back_in = {"even": back_in_even, "middle": back_in_middle, "odd": back_in_odd}
    keep = {"even": keep_even, "middle": keep_middle, "odd": keep_odd}
    loads[0].wait()
    part = span_quarters(v_ref, 4 * quarter // 128)
    for n, kind in enumerate(ORDER):
        if n == 0 or (kind == "odd") != (ORDER[n - 1] == "odd"):
            at = 2 if kind == "odd" else 1
            if loads[at] is not None:
                loads[at].wait()
                loads[at] = None
        span_chunk(kind, share, part, span_table[kind], span_out[kind])
        if n == 0:
            pl.semaphore_wait(barrier, count - 1)
        source, owners = span_out[kind], count if kind == "odd" else half
        swap(
            kind,
            everyone,
            lambda s: source.at[place[s] % owners],
            span_in.at[n, me],
            source.at[me % owners],
        )
    for load in loads[3:]:
        load.wait()
    cells = float(4 * quarter * 4 * w_ref.shape[1])
    sign = (1 - 2 * (me // half)).astype(jnp.float32)
    for n, kind in enumerate(ORDER):
        arrive(kind)
        source, target = back_out[kind], back_in[kind]

        def send(i):
            rows = slice(None)
            if kind == ORDER[-1] and False:
                rows = slice(i * 2 * share, (i + 1) * 2 * share)
            elif i < parts - 1:
                return
            if kind == "odd":
                swap(kind + "-back", everyone, lambda s: source.at[place[s], rows], target.at[me, rows], source.at[me, rows])
            else:
                swap(
                    kind + "-back" + (str(i) if kind == ORDER[-1] and False else ""),
                    beside,
                    lambda s: source.at[place[s] % half, rows],
                    target.at[my_owner, rows],
                    source.at[my_owner, rows],
                )

        stream_stage(
            share,
            py_count,
            my_owner == 0 if kind == "even" else None,
            None if kind == "odd" else sign,
            band_ref,
            span_in.at[n],
            t_h,
            t_l,
            w_ref,
            cells,
            source,
            send,
        )
    groups, _, width, _ = out_ref.shape
    done = []
    for kind in BACK_ORDER:
        for name in list(moves):
            if name.startswith(kind + "-back"):
                arrive(name)
        back_chunk(share, parts, back_in[kind], span_table[kind], keep[kind])
        done.append(kind)
        if len(done) == 1:
            continue
        for i in range(parts):
            rows = slice(i * 128, (i + 1) * 128)
            for j in range(4):
                span = slice(j * quarter, (j + 1) * quarter)
                terms = done if len(done) == 2 else done[2:]
                line = None
                for term in terms:
                    at = slice(quarter, 2 * quarter) if term == "odd" and j % 2 else slice(0, quarter)
                    value = keep[term][rows, at].reshape(groups, width, quarter)
                    minus = (term == "middle" and j % 2) or (term == "odd" and j >= 2)
                    if line is None and len(done) == 3:
                        line = out_ref[:, i, :, span]
                    if line is None:
                        line = -value if minus else value
                    else:
                        line = line - value if minus else line + value
                out_ref[:, i, :, span] = line
    for _, copies in moves.values():
        for copy in copies:
            copy.wait_send()


def register_device(velocity, band_of):
    px_count = lax.axis_size("px")
    py_count = lax.axis_size("py")
    count = px_count * py_count
    _, rows_x, _, span = velocity.shape
    stream = rows_x * px_count
    half, quarter = count // 2, span // 4
    share = quarter // count
    width = stream // count
    groups = 128 // width
    parts = len(PAIR_LIST) * NB // groups
    vmem = pl.BlockSpec(memory_space=pltpu.VMEM)
    far = pl.BlockSpec(memory_space=pltpu.HBM)
    e_h, e_l, m_h, m_l, o_h, o_l = span_tables(span)
    t_h, t_l, twiddle = stream_tables(stream)
    even = [np.concatenate(pair, 1) for pair in ((e_h, m_h), (e_l, m_l))]
    tables = np.concatenate(even + [o_h, o_l, t_h, t_l], 0)
    strips = velocity.size // 128
    rows_in, rows_back = 3 * share, 2 * parts * share
    spans = [(half, rows_in, 128), (half, rows_in, 128), (count, rows_in, 128), (3, count, rows_in, 128)]
    backs = [(n, rows_back, 128) for n in (half, half, count)]
    keeps = [(parts * 128, n * quarter) for n in (1, 1, 2)]
    lanes = 6 + parts
    operands = (band_of, velocity.reshape(strips, 128), jnp.asarray(tables), jnp.asarray(twiddle))
    out = pl.pallas_call(
        functools.partial(whole_kernel, px_count, py_count, share, parts),
        out_shape=jax.ShapeDtypeStruct((groups, parts, width, span), jnp.float32),
        in_specs=[far] * 4,
        out_specs=vmem,
        scratch_shapes=[
            pltpu.SMEM(band_of.shape, band_of.dtype),
            pltpu.VMEM((strips, 128), jnp.float32),
            pltpu.VMEM(twiddle.shape, jnp.float32),
            pltpu.VMEM(tables.shape, tables.dtype),
        ]
        + [pltpu.VMEM(shape, jnp.float32) for shape in spans + backs + backs + keeps]
        + [
            pltpu.SemaphoreType.DMA((lanes, count)),
            pltpu.SemaphoreType.DMA((lanes, count)),
            pltpu.SemaphoreType.DMA((lanes,)),
            pltpu.SemaphoreType.DMA((6,)),
        ],
        compiler_params=pltpu.CompilerParams(
            collective_id=0, has_side_effects=True, vmem_limit_bytes=49152 * 1024
        ),
    )(*[pltpu.with_memory_space_constraint(value, pltpu.HBM) for value in operands])
    return out.reshape(len(PAIR_LIST), NB, width, span)


def fills_registers(velocity, px_count, py_count):
    comps, rows_x, planes, span = velocity.shape
    count = px_count * py_count
    stream = rows_x * px_count
    share = span // 2 // count
    width = max(stream // count, 1)
    return (
        comps == 3
        and rows_x == 64
        and planes == 1
        and px_count & (px_count - 1) == 0
        and py_count & (py_count - 1) == 0
        and px_count % 8 == 0
        and span % 1024 == 0
        and stream == span
        and stream == width * count
        and planes * py_count == NB
        and NB == 2
        and span == 2 * share * count
        and share == 16
        and width == 32
        and 128 % width == 0
        and len(PAIR_LIST) * NB * width % 128 == 0
    )


def per_device(velocity, band_of):
    if fills_registers(velocity, lax.axis_size("px"), lax.axis_size("py")):
        return register_device(velocity, band_of)
    return general_device(velocity, band_of)


def solution(mesh):
    in_specs = (P(None, "px", "py", None), P())
    out_specs = P(None, None, ("px", "py"), None)
    return jax.shard_map(
        per_device, mesh=mesh, in_specs=in_specs, out_specs=out_specs, check_vma=False
    )
```

```python
import functools
import math

import jax
import jax.numpy as jnp
import numpy as np
from jax import lax
from jax.experimental import pallas as pl
from jax.experimental.pallas import tpu as pltpu
from jax.sharding import PartitionSpec as P

NB = 2


PAIR_LIST = ((0, 0), (0, 1), (0, 2), (1, 1), (1, 2), (2, 2))


def phase_table(row_values, offset, count, length):
    col_values = offset + lax.iota(jnp.int32, count)
    phase = row_values[:, None] * col_values[None, :] % length
    angle = phase.astype(jnp.float32) * (2.0 * math.pi / length)
    return (jnp.cos(angle), jnp.sin(angle))


def transform_last(real_part, imag_part, sign):
    full_shape = real_part.shape
    length = full_shape[-1]
    stacked = jnp.concatenate((real_part.reshape(-1, length), imag_part.reshape(-1, length)), 0)
    row_count = stacked.shape[0] // 2
    row_values = lax.iota(jnp.int32, length)

    def one_block(block_index, outputs):
        offset = (block_index * 128).astype(jnp.int32)
        cosine_table, sine_table = phase_table(row_values, offset, 128, length)
        with_cos = jnp.dot(
            stacked,
            cosine_table,
            precision=lax.Precision.HIGHEST,
            preferred_element_type=jnp.float32,
        )
        with_sin = jnp.dot(
            stacked, sine_table, precision=lax.Precision.HIGHEST, preferred_element_type=jnp.float32
        )
        new_real = with_cos[:row_count] - sign * with_sin[row_count:]
        new_imag = with_cos[row_count:] + sign * with_sin[:row_count]
        return (
            lax.dynamic_update_slice_in_dim(outputs[0], new_real, offset, 1),
            lax.dynamic_update_slice_in_dim(outputs[1], new_imag, offset, 1),
        )

    zeros = jnp.zeros((row_count, length), jnp.float32)
    out_real, out_imag = lax.fori_loop(0, length // 128, one_block, (zeros, zeros))
    return (out_real.reshape(full_shape), out_imag.reshape(full_shape))


def span_forward(velocity):
    comps, rows_x, planes, length = velocity.shape
    half = length // 2
    row_values = lax.iota(jnp.int32, length)

    def one_block(block_index, outputs):
        offset = (block_index * 128).astype(jnp.int32)
        cosine_table, sine_table = phase_table(row_values, offset, 128, length)
        with_cos = jnp.einsum(
            "cxpz,zk->cpkx",
            velocity,
            cosine_table,
            precision=lax.Precision.HIGHEST,
            preferred_element_type=jnp.float32,
        )
        with_sin = jnp.einsum(
            "cxpz,zk->cpkx",
            velocity,
            sine_table,
            precision=lax.Precision.HIGHEST,
            preferred_element_type=jnp.float32,
        )
        return (
            lax.dynamic_update_slice_in_dim(outputs[0], with_cos, offset, 2),
            lax.dynamic_update_slice_in_dim(outputs[1], -with_sin, offset, 2),
        )

    zeros = jnp.zeros((comps, planes, half, rows_x), jnp.float32)
    return lax.fori_loop(0, half // 128, one_block, (zeros, zeros))


def span_inverse(summed, kz_order):
    half = summed.shape[3]
    length = 2 * half
    multiplier = jnp.where(kz_order == 0, 1.0, 2.0).astype(jnp.float32)
    held_real = summed[:, :, 0] * multiplier[:, None]
    held_imag = summed[:, :, 1] * multiplier[:, None]

    def one_block(block_index, output):
        offset = (block_index * 128).astype(jnp.int32)
        cosine_table, sine_table = phase_table(kz_order, offset, 128, length)
        part = jnp.einsum(
            "sbkd,kz->sbdz",
            held_real,
            cosine_table,
            precision=lax.Precision.HIGHEST,
            preferred_element_type=jnp.float32,
        )
        part = part - jnp.einsum(
            "sbkd,kz->sbdz",
            held_imag,
            sine_table,
            precision=lax.Precision.HIGHEST,
            preferred_element_type=jnp.float32,
        )
        return lax.dynamic_update_slice_in_dim(output, part, offset, 3)

    zeros = jnp.zeros((summed.shape[0], summed.shape[1], summed.shape[4], length), jnp.float32)
    return lax.fori_loop(0, length // 128, one_block, zeros)


def general_device(velocity, band_of):
    px_count = lax.axis_size("px")
    py_count = lax.axis_size("py")
    comps, rows_x, planes, span = velocity.shape
    stream = rows_x * px_count
    half = span // 2
    local_k = half // px_count
    span_real, span_imag = span_forward(velocity)
    planes_spec = jnp.stack((span_real, span_imag), 1)
    kz_index = lax.iota(jnp.int32, local_k)
    kx_index = lax.iota(jnp.int32, stream)
    at_anchor = jnp.logical_and(
        lax.axis_index("px") == 0, jnp.logical_and(kz_index[:, None] == 0, kx_index[None, :] == 0)
    )
    keep_mask = 1.0 - at_anchor.astype(jnp.float32)
    received = lax.all_to_all(planes_spec, "px", split_axis=3, concat_axis=4, tiled=True)
    front_real, front_imag = transform_last(received[:, 0], received[:, 1], -1.0)
    spectrum = jnp.stack((front_real * keep_mask, front_imag * keep_mask), 1)
    cross_list = []
    for left_comp, right_comp in PAIR_LIST:
        left_real, left_imag = (spectrum[left_comp, 0], spectrum[left_comp, 1])
        right_real, right_imag = (spectrum[right_comp, 0], spectrum[right_comp, 1])
        cross_list.append(
            jnp.stack(
                (
                    left_real * right_real + left_imag * right_imag,
                    left_real * right_imag - left_imag * right_real,
                ),
                0,
            )
        )
    cross = jnp.stack(cross_list, 0)
    band_ids = lax.iota(jnp.int32, NB)
    onehot_all = (band_of[:, None] == band_ids[None, :]).astype(jnp.float32)
    counts = jnp.sum(onehot_all, 0)
    cells = float(stream * span)
    plane_start = lax.axis_index("py") * planes
    local_hot = lax.dynamic_slice_in_dim(onehot_all, plane_start, planes, 0)
    band_weight = local_hot / (counts[None, :] * (cells * math.sqrt(cells)))
    banded = jnp.einsum("sapkx,pb->sbakx", cross, band_weight, precision=lax.Precision.HIGHEST)
    summed = lax.psum_scatter(banded, "py", scatter_dimension=3, tiled=True)
    back_real, back_imag = transform_last(summed[:, :, 0], summed[:, :, 1], 1.0)
    exchanged = lax.all_to_all(
        lax.all_to_all(
            jnp.stack((back_real, back_imag), 2), "px", split_axis=4, concat_axis=3, tiled=True
        ),
        "py",
        split_axis=4,
        concat_axis=3,
        tiled=True,
    )
    quarter = local_k // py_count
    position = lax.iota(jnp.int32, half)
    outer = position // (px_count * quarter)
    remain = position % (px_count * quarter)
    kz_order = remain // quarter * local_k + outer * quarter + remain % quarter
    return span_inverse(exchanged, kz_order)


def split_table(table):
    high = table.astype(jnp.bfloat16)
    low = (table - high.astype(np.float64)).astype(jnp.bfloat16)
    return high, low


def span_tables(length):
    quarter, eighth = length // 4, length // 8
    column = np.arange(quarter)

    def angle(first, count):
        wave = 4 * np.arange(count) + first
        return 2.0 * np.pi * ((wave[:, None] * column[None, :]) % length) / length

    even = angle(0, eighth)
    middle = angle(2, eighth)
    odd = angle(1, quarter)
    table_even = np.concatenate((np.cos(even), -np.sin(even)), 0)
    table_middle = np.concatenate((np.cos(middle), -np.sin(middle)), 0)
    table_odd = np.block([[np.cos(odd), -np.sin(odd)], [-np.sin(odd), -np.cos(odd)]])
    return split_table(table_even) + split_table(table_middle) + split_table(table_odd)


def stream_tables(length):
    quarter = length // 4
    index = np.arange(quarter)
    angle = 2.0 * np.pi * ((index[:, None] * index[None, :]) % quarter) / quarter
    cosine, sine = np.cos(angle), np.sin(angle)
    twist = 2.0 * np.pi * (np.arange(4)[:, None] * index[None, :]) / length
    twiddle = np.concatenate((np.cos(twist), np.sin(twist)), 0).astype(np.float32)
    return split_table(np.block([[cosine, -sine], [sine, cosine]])) + (twiddle,)


def split_value(value):
    high = value.astype(jnp.bfloat16)
    low = (value - high.astype(jnp.float32)).astype(jnp.bfloat16)
    return high, low


def one_dot(left, right, dims):
    return lax.dot_general(left, right, (dims, ((), ())), preferred_element_type=jnp.float32)


NT = ((1,), (1,))
NN = ((1,), (0,))


def rows_by_table(value, table):
    high, low = split_value(value)
    rows = value.shape[0]
    by_high = one_dot(jnp.concatenate((high, low), 0), table[0], NN)
    return by_high[:rows] + (by_high[rows:] + one_dot(high, table[1], NN))


def table_by_rows(table, value):
    high, low = split_value(value)
    return one_dot(table[0], high, NT) + (
        one_dot(table[1], high, NT) + one_dot(table[0], low, NT)
    )


def span_quarters(v_ref, strips):
    rows = v_ref.shape[0] // strips
    first = rows // 3 * 2

    def strip(j):
        values = v_ref[pl.ds(j, rows, stride=strips), :]
        return jnp.concatenate((values, values[first:]), 0)

    per = strips // 4
    return [
        jnp.concatenate([strip(i * per + n) for n in range(per)], 1) for i in range(4)
    ]


def span_chunk(kind, share, part, table, out_ref):
    if kind == "odd":
        value = jnp.concatenate((part[0] - part[2], part[1] - part[3]), 1)
    else:
        ahead, behind = part[0] + part[2], part[1] + part[3]
        value = ahead + behind if kind == "even" else ahead - behind
    both = table_by_rows((table[0][...], table[1][...]), value)
    count = both.shape[0] // 2
    real, imag = both[:count], both[count:]
    lane = lax.broadcasted_iota(jnp.int32, (count, 128), 1)
    third = jnp.where(lane < 64, real[:, 128:], imag[:, 128:])
    out_ref[:, :share] = real[:, :128].reshape(-1, share, 128)
    out_ref[:, share : 2 * share] = imag[:, :128].reshape(-1, share, 128)
    out_ref[:, 2 * share :] = third.reshape(-1, share, 128)


def lane_exchange(tiles, width):
    tiles = list(tiles)
    lane = lax.broadcasted_iota(jnp.int32, tiles[0].shape, 1)
    step, size = len(tiles) // 2, 64
    while step:
        mask = lane // size % 2 == 0
        for g in range(len(tiles)):
            if g & step == 0:
                a, b = tiles[g], tiles[g + step]
                tiles[g] = jnp.where(mask, a, pltpu.roll(b, size, 1))
                tiles[g + step] = jnp.where(mask, pltpu.roll(a, 128 - size, 1), b)
        step, size = step // 2, size // 2
    return tiles


def stream_stage(share, planes, owns_mean, sign, band_ref, in_ref, t_h, t_l, w_ref, cells, out_ref):
    px_count = in_ref.shape[0] // planes
    columns = px_count // 2
    group_cols = columns // 4
    quarter = w_ref.shape[1]
    lane = lax.broadcasted_iota(jnp.int32, (3 * share, 128), 1)
    low_half = lane < 64
    blocks = []
    for q in range(columns):
        real, imag = [[], [], []], [[], [], []]
        for y in range(planes):
            a = in_ref[2 * q * planes + y]
            b = in_ref[(2 * q + 1) * planes + y]
            low = jnp.where(low_half, a, pltpu.roll(b, 64, 1))
            high = jnp.where(low_half, pltpu.roll(a, 64, 1), b)
            real[0].append(low[:share])
            imag[0].append(low[share : 2 * share])
            real[1].append(high[:share])
            imag[1].append(high[share : 2 * share])
            real[2].append(low[2 * share :])
            imag[2].append(high[2 * share :])
        blocks.append(
            (
                jnp.concatenate(real[0] + real[1] + real[2], 0),
                jnp.concatenate(imag[0] + imag[1] + imag[2], 0),
            )
        )
    part = [
        tuple(
            jnp.concatenate([blocks[j * group_cols + g][ri] for g in range(group_cols)], 1)
            for ri in range(2)
        )
        for j in range(4)
    ]

    def cross4(v):
        s02 = [v[0][i] + v[2][i] for i in range(2)]
        d02 = [v[0][i] - v[2][i] for i in range(2)]
        s13 = [v[1][i] + v[3][i] for i in range(2)]
        d13 = [v[1][i] - v[3][i] for i in range(2)]
        return [
            (s02[0] + s13[0], s02[1] + s13[1]),
            (d02[0] + d13[1], d02[1] - d13[0]),
            (s02[0] - s13[0], s02[1] - s13[1]),
            (d02[0] - d13[1], d02[1] + d13[0]),
        ]

    turned = []
    for k1, (real, imag) in enumerate(cross4(part)):
        if k1:
            cosine, sine = w_ref[k1 : k1 + 1], w_ref[4 + k1 : 5 + k1]
            real, imag = real * cosine + imag * sine, imag * cosine - real * sine
        turned.append(jnp.concatenate((real, imag), 1))
    table = (t_h[...], t_l[...])
    front = rows_by_table(jnp.concatenate(turned, 0), table)
    if owns_mean is not None:
        block = 3 * planes * share
        row = lax.broadcasted_iota(jnp.int32, (block, 2 * quarter), 0)
        col = lax.broadcasted_iota(jnp.int32, (block, 2 * quarter), 1)
        anchor = jnp.logical_and(row % share == 0, col % quarter == 0)
        anchor = jnp.logical_and(anchor, owns_mean)
        front = jnp.concatenate((jnp.where(anchor, 0.0, front[:block]), front[block:]), 0)
    front = front.reshape(4, 3, planes, share, 2 * quarter)
    tall = (4 * share, quarter)

    def spectrum(c, y, ri):
        return front[:, c, y, :, ri * quarter : (ri + 1) * quarter].reshape(tall)

    in_order = jnp.full(tall, band_ref[0], jnp.int32) == 0
    field = [
        [
            tuple(
                jnp.where(in_order, spectrum(c, b, ri), spectrum(c, 1 - b, ri)) for ri in range(2)
            )
            for b in range(NB)
        ]
        for c in range(3)
    ]
    scale = 2.0 / (cells * math.sqrt(cells))
    if owns_mean is not None:
        row = lax.broadcasted_iota(jnp.int32, tall, 0)
        single = jnp.logical_and(row % share == 0, owns_mean)
        scale = jnp.where(single, 0.5 * scale, scale)

    def banded(left, right, b):
        lr, li = field[left][b]
        rr, ri = field[right][b]
        real = (lr * rr + li * ri) * scale
        if left == right:
            return real
        return jnp.concatenate((real, (li * rr - lr * ri) * scale), 1)

    members = list(range(len(PAIR_LIST) * NB))
    lines = [None] * len(members)
    own_table = (t_h[:quarter], t_l[:quarter])
    for alike, used in ((True, own_table), (False, table)):
        chosen = [m for m in members if (len(set(PAIR_LIST[m // NB])) == 1) == alike]
        joined = jnp.concatenate([banded(*PAIR_LIST[m // NB], m % NB) for m in chosen], 0)
        whole = rows_by_table(joined, used)
        for at, m in enumerate(chosen):
            back = whole[at * 4 * share : (at + 1) * 4 * share]
            turned = []
            for k1 in range(4):
                real = back[k1 * share : (k1 + 1) * share, :quarter]
                imag = back[k1 * share : (k1 + 1) * share, quarter:]
                if k1:
                    cosine, sine = w_ref[k1 : k1 + 1], w_ref[4 + k1 : 5 + k1]
                    if sign is not None and k1 % 2:
                        cosine, sine = cosine * sign, sine * sign
                    real, imag = real * cosine + imag * sine, imag * cosine - real * sine
                turned.append((real, imag))
            lines[m] = cross4(turned)
    held = 4 * quarter if sign is None else 2 * quarter
    width = held // out_ref.shape[0]
    groups = 128 // width
    per_group = len(members) // groups
    for i in range(per_group):
        for ri in range(2):
            at = (i * 2 + ri) * share
            for q in range(held // 128):
                j, inside = q * 128 // quarter, q * 128 % quarter
                tiles = [
                    lines[g * per_group + i][j][ri][:, inside : inside + 128]
                    for g in range(groups)
                ]
                for t, packed in enumerate(lane_exchange(tiles, width)):
                    out_ref[q * groups + t, at : at + share] = packed


def back_chunk(share, parts, in_ref, table):
    sources = in_ref.shape[0]

    def turned(i, ri):
        at = (i * 2 + ri) * share
        return in_ref[:, at : at + share].reshape(sources * share, 128).T

    value = jnp.concatenate(
        [jnp.concatenate((turned(i, 0), -turned(i, 1)), 1) for i in range(parts)], 0
    )
    return rows_by_table(value, table)


def flip_bits(index, bits):
    moved, bit = index, 1
    while bit <= bits:
        if bits & bit:
            moved = moved + bit * (1 - 2 * ((index // bit) % 2))
        bit *= 2
    return moved


ORDER = ("even", "odd", "middle")
SEND_ORDER = "xx nf nd"


def whole_kernel(
    px_count,
    py_count,
    share,
    parts,
    band_far,
    v_far,
    table_far,
    w_far,
    out_ref,
    band_ref,
    v_ref,
    w_ref,
    tables,
    span_out_even,
    span_out_middle,
    span_out_odd,
    span_in,
    back_out_even,
    back_out_middle,
    back_out_odd,
    back_in_even,
    back_in_middle,
    back_in_odd,
    keep_even,
    keep_middle,
    send_sem,
    recv_sem,
    load_sem,
):
    quarter = tables.shape[1] // 2
    cuts = (0, 2 * quarter, 6 * quarter, 10 * quarter)
    pairs = [(v_far, v_ref)]
    pairs += [
        (table_far.at[start:stop], tables.at[start:stop])
        for start, stop in zip(cuts[:-1], cuts[1:])
    ]
    pairs += [(w_far, w_ref), (band_far, band_ref)]
    loads = [
        pltpu.make_async_copy(source, target, load_sem.at[n])
        for n, (source, target) in enumerate(pairs)
    ]
    span_table = {
        "even": [tables.at[n * quarter : (n + 1) * quarter, :quarter] for n in range(2)],
        "middle": [tables.at[n * quarter : (n + 1) * quarter, quarter:] for n in range(2)],
        "odd": [tables.at[n * quarter : (n + 2) * quarter] for n in (2, 4)],
    }
    t_h, t_l = tables.at[6 * quarter : 8 * quarter], tables.at[8 * quarter :]
    px, py = lax.axis_index("px"), lax.axis_index("py")
    count = px_count * py_count
    half = count // 2
    me = px * py_count + py
    my_owner = me % half
    barrier = pltpu.get_barrier_semaphore()
    near, far = list(range(1, half)), list(range(half, count))
    peers = {
        s: (flip_bits(px, s // py_count), flip_bits(py, s % py_count)) for s in near + far
    }
    place = {s: peers[s][0] * py_count + peers[s][1] for s in peers}
    for s in far + near:
        pl.semaphore_signal(
            barrier, inc=1, device_id=peers[s], device_id_type=pl.DeviceIdType.MESH
        )
    for load in loads:
        load.start()
    moves = {}

    def swap(name, steps, source_at, target, own_source):
        lane = len(moves)
        for s in steps:
            pltpu.make_async_remote_copy(
                src_ref=source_at(s),
                dst_ref=target,
                send_sem=send_sem.at[lane],
                recv_sem=recv_sem.at[lane, int(s >= half)],
                device_id=peers[s],
                device_id_type=pl.DeviceIdType.MESH,
            ).start()
        pltpu.make_async_copy(own_source, target, recv_sem.at[lane, 0]).start()
        moves[name] = (lane, len(steps))

    def arrive(name, into, sides=(0, 1)):
        for side in sides:
            slots = into.at[:half]
            pltpu.make_async_copy(slots, slots, recv_sem.at[moves[name][0], side]).wait()

    def sent(name, into):
        lane, copies = moves[name]
        slots = into.at[:copies]
        pltpu.make_async_copy(slots, slots, send_sem.at[lane]).wait()

    orders = {
        "nf": near + far,
        "fn": far + near,
        "dn": (near + far)[::-1],
        "nu": near,
        "nd": near[::-1],
        "xx": near[::-1] + far[::-1],
    }
    first_order, last_order, beside = (orders[name] for name in SEND_ORDER.split())
    span_out = {"even": span_out_even, "middle": span_out_middle, "odd": span_out_odd}
    back_out = {"even": back_out_even, "middle": back_out_middle, "odd": back_out_odd}
    back_in = {"even": back_in_even, "middle": back_in_middle, "odd": back_in_odd}
    keep = {"even": keep_even, "middle": keep_middle}
    loads[0].wait()
    part = span_quarters(v_ref, 4 * quarter // 128)
    for n, kind in enumerate(ORDER):
        if n == 0 or (kind == "odd") != (ORDER[n - 1] == "odd"):
            at = 2 if kind == "odd" else 1
            if loads[at] is not None:
                loads[at].wait()
                loads[at] = None
        span_chunk(kind, share, part, span_table[kind], span_out[kind])
        if n == 0:
            pl.semaphore_wait(barrier, count - 1)
        source, owners = span_out[kind], count if kind == "odd" else half
        swap(
            kind,
            first_order,
            lambda s: source.at[place[s] % owners],
            span_in.at[n, me],
            source.at[me % owners],
        )
    for load in loads[3:]:
        load.wait()
    cells = float(4 * quarter * 4 * w_ref.shape[1])
    sign = (1 - 2 * (me // half)).astype(jnp.float32)
    for n, kind in enumerate(ORDER):
        arrive(kind, span_in.at[n])
        source, target = back_out[kind], back_in[kind]

        def send():
            if kind == "odd":
                swap(
                    kind + "-back",
                    last_order,
                    lambda s: source.at[place[s]],
                    target.at[me],
                    source.at[me],
                )
            else:
                swap(
                    kind + "-back",
                    beside,
                    lambda s: source.at[place[s] % half],
                    target.at[my_owner],
                    source.at[my_owner],
                )

        stream_stage(
            share,
            py_count,
            my_owner == 0 if kind == "even" else None,
            None if kind == "odd" else sign,
            band_ref,
            span_in.at[n],
            t_h,
            t_l,
            w_ref,
            cells,
            source,
        )
        send()
    groups, _, width, _ = out_ref.shape

    def spread(i, j, value):
        out_ref[:, i, :, j * quarter : (j + 1) * quarter] = value.reshape(groups, width, quarter)

    def spread_more(i, j, value):
        at = slice(j * quarter, (j + 1) * quarter)
        out_ref[:, i, :, at] = out_ref[:, i, :, at] + value.reshape(groups, width, quarter)

    for kind in ("even", "middle"):
        arrive(kind + "-back", back_in[kind], (0,))
        table = [side[...] for side in span_table[kind]]
        keep[kind][...] = back_chunk(share, parts, back_in[kind], table)
    for i in range(parts):
        rows = slice(i * 128, (i + 1) * 128)
        for j in range(2):
            value = keep_even[rows] - keep_middle[rows] if j else keep_even[rows] + keep_middle[rows]
            spread(i, j, value)
            spread(i, j + 2, value)
    side_of_me = me // half
    for steps, side in ((near, side_of_me), (far, 1 - side_of_me)):
        if steps is far:
            for n, kind in enumerate(ORDER):
                sent(kind, span_in.at[n])
            for kind in ("even", "middle"):
                sent(kind + "-back", back_in[kind])
        arrive("odd-back", back_in_odd, (int(steps is far),))
        first = pl.multiple_of(side * half, half)
        wave = pl.multiple_of(side * half * share, half * share)
        table = [
            jnp.concatenate(
                [ref[pl.ds(at + wave, half * share)] for at in (0, quarter)], 0
            )
            for ref in span_table["odd"]
        ]
        source = back_in_odd.at[pl.ds(first, half)]
        both = back_chunk(share, parts, source, table)
        for i in range(parts):
            rows = slice(i * 128, (i + 1) * 128)
            for j in range(4):
                value = both[rows, (j % 2) * quarter : (j % 2 + 1) * quarter]
                spread_more(i, j, value if j < 2 else -value)
    sent("odd-back", back_in_odd)


def register_device(velocity, band_of):
    px_count = lax.axis_size("px")
    py_count = lax.axis_size("py")
    count = px_count * py_count
    _, rows_x, _, span = velocity.shape
    stream = rows_x * px_count
    half, quarter = count // 2, span // 4
    share = quarter // count
    width = stream // count
    groups = 128 // width
    parts = len(PAIR_LIST) * NB // groups
    vmem = pl.BlockSpec(memory_space=pltpu.VMEM)
    far = pl.BlockSpec(memory_space=pltpu.HBM)
    e_h, e_l, m_h, m_l, o_h, o_l = span_tables(span)
    t_h, t_l, twiddle = stream_tables(stream)
    even = [np.concatenate(pair, 1) for pair in ((e_h, m_h), (e_l, m_l))]
    tables = np.concatenate(even + [o_h, o_l, t_h, t_l], 0)
    strips = velocity.size // 128
    rows_in, rows_back = 3 * share, 2 * parts * share
    spans = [(half, rows_in, 128), (half, rows_in, 128), (count, rows_in, 128), (3, count, rows_in, 128)]
    backs = [(n, rows_back, 128) for n in (half, half, count)]
    keeps = [(parts * 128, n * quarter) for n in (1, 1)]
    lanes = 6
    operands = (band_of, velocity.reshape(strips, 128), jnp.asarray(tables), jnp.asarray(twiddle))
    out = pl.pallas_call(
        functools.partial(whole_kernel, px_count, py_count, share, parts),
        out_shape=jax.ShapeDtypeStruct((groups, parts, width, span), jnp.float32),
        in_specs=[far] * 4,
        out_specs=vmem,
        scratch_shapes=[
            pltpu.SMEM(band_of.shape, band_of.dtype),
            pltpu.VMEM((strips, 128), jnp.float32),
            pltpu.VMEM(twiddle.shape, jnp.float32),
            pltpu.VMEM(tables.shape, tables.dtype),
        ]
        + [pltpu.VMEM(shape, jnp.float32) for shape in spans + backs + backs + keeps]
        + [
            pltpu.SemaphoreType.DMA((lanes,)),
            pltpu.SemaphoreType.DMA((lanes, 2)),
            pltpu.SemaphoreType.DMA((6,)),
        ],
        compiler_params=pltpu.CompilerParams(
            collective_id=0, has_side_effects=True, vmem_limit_bytes=49152 * 1024
        ),
    )(*[pltpu.with_memory_space_constraint(value, pltpu.HBM) for value in operands])
    return out.reshape(len(PAIR_LIST), NB, width, span)


def fills_registers(velocity, px_count, py_count):
    comps, rows_x, planes, span = velocity.shape
    count = px_count * py_count
    stream = rows_x * px_count
    share = span // 2 // count
    width = max(stream // count, 1)
    return (
        comps == 3
        and rows_x == 64
        and planes == 1
        and px_count & (px_count - 1) == 0
        and py_count & (py_count - 1) == 0
        and px_count % 8 == 0
        and span % 1024 == 0
        and stream == span
        and stream == width * count
        and planes * py_count == NB
        and NB == 2
        and span == 2 * share * count
        and share == 16
        and width == 32
        and 128 % width == 0
        and len(PAIR_LIST) * NB * width % 128 == 0
    )


def per_device(velocity, band_of):
    if fills_registers(velocity, lax.axis_size("px"), lax.axis_size("py")):
        return register_device(velocity, band_of)
    return general_device(velocity, band_of)


def solution(mesh):
    in_specs = (P(None, "px", "py", None), P())
    out_specs = P(None, None, ("px", "py"), None)
    return jax.shard_map(
        per_device, mesh=mesh, in_specs=in_specs, out_specs=out_specs, check_vma=False
    )
```

```python
import functools
import math

import jax
import jax.numpy as jnp
import numpy as np
from jax import lax
from jax.experimental import pallas as pl
from jax.experimental.pallas import tpu as pltpu
from jax.sharding import PartitionSpec as P

NB = 2


PAIR_LIST = ((0, 0), (0, 1), (0, 2), (1, 1), (1, 2), (2, 2))


def phase_table(row_values, offset, count, length):
    col_values = offset + lax.iota(jnp.int32, count)
    phase = row_values[:, None] * col_values[None, :] % length
    angle = phase.astype(jnp.float32) * (2.0 * math.pi / length)
    return (jnp.cos(angle), jnp.sin(angle))


def transform_last(real_part, imag_part, sign):
    full_shape = real_part.shape
    length = full_shape[-1]
    stacked = jnp.concatenate((real_part.reshape(-1, length), imag_part.reshape(-1, length)), 0)
    row_count = stacked.shape[0] // 2
    row_values = lax.iota(jnp.int32, length)

    def one_block(block_index, outputs):
        offset = (block_index * 128).astype(jnp.int32)
        cosine_table, sine_table = phase_table(row_values, offset, 128, length)
        with_cos = jnp.dot(
            stacked,
            cosine_table,
            precision=lax.Precision.HIGHEST,
            preferred_element_type=jnp.float32,
        )
        with_sin = jnp.dot(
            stacked, sine_table, precision=lax.Precision.HIGHEST, preferred_element_type=jnp.float32
        )
        new_real = with_cos[:row_count] - sign * with_sin[row_count:]
        new_imag = with_cos[row_count:] + sign * with_sin[:row_count]
        return (
            lax.dynamic_update_slice_in_dim(outputs[0], new_real, offset, 1),
            lax.dynamic_update_slice_in_dim(outputs[1], new_imag, offset, 1),
        )

    zeros = jnp.zeros((row_count, length), jnp.float32)
    out_real, out_imag = lax.fori_loop(0, length // 128, one_block, (zeros, zeros))
    return (out_real.reshape(full_shape), out_imag.reshape(full_shape))


def span_forward(velocity):
    comps, rows_x, planes, length = velocity.shape
    half = length // 2
    row_values = lax.iota(jnp.int32, length)

    def one_block(block_index, outputs):
        offset = (block_index * 128).astype(jnp.int32)
        cosine_table, sine_table = phase_table(row_values, offset, 128, length)
        with_cos = jnp.einsum(
            "cxpz,zk->cpkx",
            velocity,
            cosine_table,
            precision=lax.Precision.HIGHEST,
            preferred_element_type=jnp.float32,
        )
        with_sin = jnp.einsum(
            "cxpz,zk->cpkx",
            velocity,
            sine_table,
            precision=lax.Precision.HIGHEST,
            preferred_element_type=jnp.float32,
        )
        return (
            lax.dynamic_update_slice_in_dim(outputs[0], with_cos, offset, 2),
            lax.dynamic_update_slice_in_dim(outputs[1], -with_sin, offset, 2),
        )

    zeros = jnp.zeros((comps, planes, half, rows_x), jnp.float32)
    return lax.fori_loop(0, half // 128, one_block, (zeros, zeros))


def span_inverse(summed, kz_order):
    half = summed.shape[3]
    length = 2 * half
    multiplier = jnp.where(kz_order == 0, 1.0, 2.0).astype(jnp.float32)
    held_real = summed[:, :, 0] * multiplier[:, None]
    held_imag = summed[:, :, 1] * multiplier[:, None]

    def one_block(block_index, output):
        offset = (block_index * 128).astype(jnp.int32)
        cosine_table, sine_table = phase_table(kz_order, offset, 128, length)
        part = jnp.einsum(
            "sbkd,kz->sbdz",
            held_real,
            cosine_table,
            precision=lax.Precision.HIGHEST,
            preferred_element_type=jnp.float32,
        )
        part = part - jnp.einsum(
            "sbkd,kz->sbdz",
            held_imag,
            sine_table,
            precision=lax.Precision.HIGHEST,
            preferred_element_type=jnp.float32,
        )
        return lax.dynamic_update_slice_in_dim(output, part, offset, 3)

    zeros = jnp.zeros((summed.shape[0], summed.shape[1], summed.shape[4], length), jnp.float32)
    return lax.fori_loop(0, length // 128, one_block, zeros)


def general_device(velocity, band_of):
    px_count = lax.axis_size("px")
    py_count = lax.axis_size("py")
    comps, rows_x, planes, span = velocity.shape
    stream = rows_x * px_count
    half = span // 2
    local_k = half // px_count
    span_real, span_imag = span_forward(velocity)
    planes_spec = jnp.stack((span_real, span_imag), 1)
    kz_index = lax.iota(jnp.int32, local_k)
    kx_index = lax.iota(jnp.int32, stream)
    at_anchor = jnp.logical_and(
        lax.axis_index("px") == 0, jnp.logical_and(kz_index[:, None] == 0, kx_index[None, :] == 0)
    )
    keep_mask = 1.0 - at_anchor.astype(jnp.float32)
    received = lax.all_to_all(planes_spec, "px", split_axis=3, concat_axis=4, tiled=True)
    front_real, front_imag = transform_last(received[:, 0], received[:, 1], -1.0)
    spectrum = jnp.stack((front_real * keep_mask, front_imag * keep_mask), 1)
    cross_list = []
    for left_comp, right_comp in PAIR_LIST:
        left_real, left_imag = (spectrum[left_comp, 0], spectrum[left_comp, 1])
        right_real, right_imag = (spectrum[right_comp, 0], spectrum[right_comp, 1])
        cross_list.append(
            jnp.stack(
                (
                    left_real * right_real + left_imag * right_imag,
                    left_real * right_imag - left_imag * right_real,
                ),
                0,
            )
        )
    cross = jnp.stack(cross_list, 0)
    band_ids = lax.iota(jnp.int32, NB)
    onehot_all = (band_of[:, None] == band_ids[None, :]).astype(jnp.float32)
    counts = jnp.sum(onehot_all, 0)
    cells = float(stream * span)
    plane_start = lax.axis_index("py") * planes
    local_hot = lax.dynamic_slice_in_dim(onehot_all, plane_start, planes, 0)
    band_weight = local_hot / (counts[None, :] * (cells * math.sqrt(cells)))
    banded = jnp.einsum("sapkx,pb->sbakx", cross, band_weight, precision=lax.Precision.HIGHEST)
    summed = lax.psum_scatter(banded, "py", scatter_dimension=3, tiled=True)
    back_real, back_imag = transform_last(summed[:, :, 0], summed[:, :, 1], 1.0)
    exchanged = lax.all_to_all(
        lax.all_to_all(
            jnp.stack((back_real, back_imag), 2), "px", split_axis=4, concat_axis=3, tiled=True
        ),
        "py",
        split_axis=4,
        concat_axis=3,
        tiled=True,
    )
    quarter = local_k // py_count
    position = lax.iota(jnp.int32, half)
    outer = position // (px_count * quarter)
    remain = position % (px_count * quarter)
    kz_order = remain // quarter * local_k + outer * quarter + remain % quarter
    return span_inverse(exchanged, kz_order)


def split_table(table):
    high = table.astype(jnp.bfloat16)
    low = (table - high.astype(np.float64)).astype(jnp.bfloat16)
    return high, low


def span_tables(length):
    quarter, eighth = length // 4, length // 8
    column = np.arange(quarter)

    def angle(first, count):
        wave = 4 * np.arange(count) + first
        return 2.0 * np.pi * ((wave[:, None] * column[None, :]) % length) / length

    even = angle(0, eighth)
    middle = angle(2, eighth)
    odd = angle(1, quarter)
    table_even = np.concatenate((np.cos(even), -np.sin(even)), 0)
    table_middle = np.concatenate((np.cos(middle), -np.sin(middle)), 0)
    table_odd = np.block([[np.cos(odd), -np.sin(odd)], [-np.sin(odd), -np.cos(odd)]])
    return split_table(table_even) + split_table(table_middle) + split_table(table_odd)


def stream_tables(length):
    quarter = length // 4
    index = np.arange(quarter)
    angle = 2.0 * np.pi * ((index[:, None] * index[None, :]) % quarter) / quarter
    cosine, sine = np.cos(angle), np.sin(angle)
    twist = 2.0 * np.pi * (np.arange(4)[:, None] * index[None, :]) / length
    twiddle = np.concatenate((np.cos(twist), np.sin(twist)), 0).astype(np.float32)
    return split_table(np.block([[cosine, -sine], [sine, cosine]])) + (twiddle,)


def split_value(value):
    high = value.astype(jnp.bfloat16)
    low = (value - high.astype(jnp.float32)).astype(jnp.bfloat16)
    return high, low


def one_dot(left, right, dims):
    return lax.dot_general(left, right, (dims, ((), ())), preferred_element_type=jnp.float32)


NT = ((1,), (1,))
NN = ((1,), (0,))


def rows_by_table(value, table):
    high, low = split_value(value)
    rows = value.shape[0]
    by_high = one_dot(jnp.concatenate((high, low), 0), table[0], NN)
    return by_high[:rows] + (by_high[rows:] + one_dot(high, table[1], NN))


def table_by_rows(table, value):
    high, low = split_value(value)
    return one_dot(table[0], high, NT) + (
        one_dot(table[1], high, NT) + one_dot(table[0], low, NT)
    )


def span_quarters(v_ref, strips):
    rows = v_ref.shape[0] // strips
    first = rows // 3 * 2

    def strip(j):
        values = v_ref[pl.ds(j, rows, stride=strips), :]
        return jnp.concatenate((values, values[first:]), 0)

    per = strips // 4
    return [
        jnp.concatenate([strip(i * per + n) for n in range(per)], 1) for i in range(4)
    ]


def span_chunk(kind, share, part, table, out_ref):
    if kind == "odd":
        value = jnp.concatenate((part[0] - part[2], part[1] - part[3]), 1)
    else:
        ahead, behind = part[0] + part[2], part[1] + part[3]
        value = ahead + behind if kind == "even" else ahead - behind
    both = table_by_rows((table[0][...], table[1][...]), value)
    count = both.shape[0] // 2
    real, imag = both[:count], both[count:]
    lane = lax.broadcasted_iota(jnp.int32, (count, 128), 1)
    third = jnp.where(lane < 64, real[:, 128:], imag[:, 128:])
    out_ref[:, :share] = real[:, :128].reshape(-1, share, 128)
    out_ref[:, share : 2 * share] = imag[:, :128].reshape(-1, share, 128)
    out_ref[:, 2 * share :] = third.reshape(-1, share, 128)


def lane_exchange(tiles, width):
    tiles = list(tiles)
    lane = lax.broadcasted_iota(jnp.int32, tiles[0].shape, 1)
    step, size = len(tiles) // 2, 64
    while step:
        mask = lane // size % 2 == 0
        for g in range(len(tiles)):
            if g & step == 0:
                a, b = tiles[g], tiles[g + step]
                tiles[g] = jnp.where(mask, a, pltpu.roll(b, size, 1))
                tiles[g + step] = jnp.where(mask, pltpu.roll(a, 128 - size, 1), b)
        step, size = step // 2, size // 2
    return tiles


def stream_stage(share, planes, owns_mean, sign, band_ref, in_ref, t_h, t_l, w_ref, cells, out_ref):
    px_count = in_ref.shape[0] // planes
    columns = px_count // 2
    group_cols = columns // 4
    quarter = w_ref.shape[1]
    lane = lax.broadcasted_iota(jnp.int32, (3 * share, 128), 1)
    low_half = lane < 64
    blocks = []
    for q in range(columns):
        real, imag = [[], [], []], [[], [], []]
        for y in range(planes):
            a = in_ref[2 * q * planes + y]
            b = in_ref[(2 * q + 1) * planes + y]
            low = jnp.where(low_half, a, pltpu.roll(b, 64, 1))
            high = jnp.where(low_half, pltpu.roll(a, 64, 1), b)
            real[0].append(low[:share])
            imag[0].append(low[share : 2 * share])
            real[1].append(high[:share])
            imag[1].append(high[share : 2 * share])
            real[2].append(low[2 * share :])
            imag[2].append(high[2 * share :])
        blocks.append(
            (
                jnp.concatenate(real[0] + real[1] + real[2], 0),
                jnp.concatenate(imag[0] + imag[1] + imag[2], 0),
            )
        )
    part = [
        tuple(
            jnp.concatenate([blocks[j * group_cols + g][ri] for g in range(group_cols)], 1)
            for ri in range(2)
        )
        for j in range(4)
    ]

    def cross4(v):
        s02 = [v[0][i] + v[2][i] for i in range(2)]
        d02 = [v[0][i] - v[2][i] for i in range(2)]
        s13 = [v[1][i] + v[3][i] for i in range(2)]
        d13 = [v[1][i] - v[3][i] for i in range(2)]
        return [
            (s02[0] + s13[0], s02[1] + s13[1]),
            (d02[0] + d13[1], d02[1] - d13[0]),
            (s02[0] - s13[0], s02[1] - s13[1]),
            (d02[0] - d13[1], d02[1] + d13[0]),
        ]

    turned = []
    for k1, (real, imag) in enumerate(cross4(part)):
        if k1:
            cosine, sine = w_ref[k1 : k1 + 1], w_ref[4 + k1 : 5 + k1]
            real, imag = real * cosine + imag * sine, imag * cosine - real * sine
        turned.append(jnp.concatenate((real, imag), 1))
    table = (t_h[...], t_l[...])
    front = rows_by_table(jnp.concatenate(turned, 0), table)
    if owns_mean is not None:
        block = 3 * planes * share
        row = lax.broadcasted_iota(jnp.int32, (block, 2 * quarter), 0)
        col = lax.broadcasted_iota(jnp.int32, (block, 2 * quarter), 1)
        anchor = jnp.logical_and(row % share == 0, col % quarter == 0)
        anchor = jnp.logical_and(anchor, owns_mean)
        front = jnp.concatenate((jnp.where(anchor, 0.0, front[:block]), front[block:]), 0)
    front = front.reshape(4, 3, planes, share, 2 * quarter)
    tall = (4 * share, quarter)

    def spectrum(c, y, ri):
        return front[:, c, y, :, ri * quarter : (ri + 1) * quarter].reshape(tall)

    in_order = jnp.full(tall, band_ref[0], jnp.int32) == 0
    field = [
        [
            tuple(
                jnp.where(in_order, spectrum(c, b, ri), spectrum(c, 1 - b, ri)) for ri in range(2)
            )
            for b in range(NB)
        ]
        for c in range(3)
    ]
    scale = 2.0 / (cells * math.sqrt(cells))
    if owns_mean is not None:
        row = lax.broadcasted_iota(jnp.int32, tall, 0)
        single = jnp.logical_and(row % share == 0, owns_mean)
        scale = jnp.where(single, 0.5 * scale, scale)

    def banded(left, right, b):
        lr, li = field[left][b]
        rr, ri = field[right][b]
        real = (lr * rr + li * ri) * scale
        if left == right:
            return real
        return jnp.concatenate((real, (li * rr - lr * ri) * scale), 1)

    members = list(range(len(PAIR_LIST) * NB))
    lines = [None] * len(members)
    own_table = (t_h[:quarter], t_l[:quarter])
    for alike, used in ((True, own_table), (False, table)):
        chosen = [m for m in members if (len(set(PAIR_LIST[m // NB])) == 1) == alike]
        joined = jnp.concatenate([banded(*PAIR_LIST[m // NB], m % NB) for m in chosen], 0)
        whole = rows_by_table(joined, used)
        for at, m in enumerate(chosen):
            back = whole[at * 4 * share : (at + 1) * 4 * share]
            turned = []
            for k1 in range(4):
                real = back[k1 * share : (k1 + 1) * share, :quarter]
                imag = back[k1 * share : (k1 + 1) * share, quarter:]
                if k1:
                    cosine, sine = w_ref[k1 : k1 + 1], w_ref[4 + k1 : 5 + k1]
                    if sign is not None and k1 % 2:
                        cosine, sine = cosine * sign, sine * sign
                    real, imag = real * cosine + imag * sine, imag * cosine - real * sine
                turned.append((real, imag))
            lines[m] = cross4(turned)
    held = 4 * quarter if sign is None else 2 * quarter
    width = held // out_ref.shape[0]
    groups = 128 // width
    per_group = len(members) // groups
    for i in range(per_group):
        for ri in range(2):
            at = (i * 2 + ri) * share
            for q in range(held // 128):
                j, inside = q * 128 // quarter, q * 128 % quarter
                tiles = [
                    lines[g * per_group + i][j][ri][:, inside : inside + 128]
                    for g in range(groups)
                ]
                for t, packed in enumerate(lane_exchange(tiles, width)):
                    out_ref[q * groups + t, at : at + share] = packed


def back_chunk(share, parts, in_ref, table):
    sources = in_ref.shape[0]

    def turned(i, ri):
        at = (i * 2 + ri) * share
        return in_ref[:, at : at + share].reshape(sources * share, 128).T

    value = jnp.concatenate(
        [jnp.concatenate((turned(i, 0), -turned(i, 1)), 1) for i in range(parts)], 0
    )
    return rows_by_table(value, table)


def flip_bits(index, bits):
    moved, bit = index, 1
    while bit <= bits:
        if bits & bit:
            moved = moved + bit * (1 - 2 * ((index // bit) % 2))
        bit *= 2
    return moved


ORDER = ("even", "odd", "middle")
SEND_ORDER = "fx xx fn nd"


def whole_kernel(
    px_count,
    py_count,
    share,
    parts,
    band_far,
    v_far,
    table_far,
    w_far,
    out_ref,
    band_ref,
    v_ref,
    w_ref,
    tables,
    span_out_even,
    span_out_middle,
    span_out_odd,
    span_in,
    back_out_even,
    back_out_middle,
    back_out_odd,
    back_in_even,
    back_in_middle,
    back_in_odd,
    keep_even,
    keep_middle,
    send_sem,
    recv_sem,
    load_sem,
):
    quarter = tables.shape[1] // 2
    cuts = (0, 2 * quarter, 6 * quarter, 10 * quarter)
    pairs = [(v_far, v_ref)]
    pairs += [
        (table_far.at[start:stop], tables.at[start:stop])
        for start, stop in zip(cuts[:-1], cuts[1:])
    ]
    pairs += [(w_far, w_ref), (band_far, band_ref)]
    loads = [
        pltpu.make_async_copy(source, target, load_sem.at[n])
        for n, (source, target) in enumerate(pairs)
    ]
    span_table = {
        "even": [tables.at[n * quarter : (n + 1) * quarter, :quarter] for n in range(2)],
        "middle": [tables.at[n * quarter : (n + 1) * quarter, quarter:] for n in range(2)],
        "odd": [tables.at[n * quarter : (n + 2) * quarter] for n in (2, 4)],
    }
    t_h, t_l = tables.at[6 * quarter : 8 * quarter], tables.at[8 * quarter :]
    px, py = lax.axis_index("px"), lax.axis_index("py")
    count = px_count * py_count
    half = count // 2
    me = px * py_count + py
    my_owner = me % half
    barrier = pltpu.get_barrier_semaphore()
    near, far = list(range(1, half)), list(range(half, count))
    peers = {
        s: (flip_bits(px, s // py_count), flip_bits(py, s % py_count)) for s in near + far
    }
    place = {s: peers[s][0] * py_count + peers[s][1] for s in peers}
    for s in far + near:
        pl.semaphore_signal(
            barrier, inc=1, device_id=peers[s], device_id_type=pl.DeviceIdType.MESH
        )
    for load in loads:
        load.start()
    moves = {}

    def swap(name, steps, source_at, target, own_source):
        lane = len(moves)
        for s in steps:
            pltpu.make_async_remote_copy(
                src_ref=source_at(s),
                dst_ref=target,
                send_sem=send_sem.at[lane],
                recv_sem=recv_sem.at[lane, int(s >= half)],
                device_id=peers[s],
                device_id_type=pl.DeviceIdType.MESH,
            ).start()
        pltpu.make_async_copy(own_source, target, recv_sem.at[lane, 0]).start()
        moves[name] = (lane, len(steps))

    def arrive(name, into, sides=(0, 1)):
        for side in sides:
            slots = into.at[:half]
            pltpu.make_async_copy(slots, slots, recv_sem.at[moves[name][0], side]).wait()

    def sent(name, into):
        lane, copies = moves[name]
        slots = into.at[:copies]
        pltpu.make_async_copy(slots, slots, send_sem.at[lane]).wait()

    orders = {
        "nf": near + far,
        "fn": far + near,
        "dn": (near + far)[::-1],
        "nu": near,
        "nd": near[::-1],
        "xx": near[::-1] + far[::-1],
        "fx": far[::-1] + near[::-1],
    }
    opening_order, first_order, last_order, beside = (
        orders[name] for name in SEND_ORDER.split()
    )
    span_out = {"even": span_out_even, "middle": span_out_middle, "odd": span_out_odd}
    back_out = {"even": back_out_even, "middle": back_out_middle, "odd": back_out_odd}
    back_in = {"even": back_in_even, "middle": back_in_middle, "odd": back_in_odd}
    keep = {"even": keep_even, "middle": keep_middle}
    loads[0].wait()
    part = span_quarters(v_ref, 4 * quarter // 128)
    for n, kind in enumerate(ORDER):
        if n == 0 or (kind == "odd") != (ORDER[n - 1] == "odd"):
            at = 2 if kind == "odd" else 1
            if loads[at] is not None:
                loads[at].wait()
                loads[at] = None
        span_chunk(kind, share, part, span_table[kind], span_out[kind])
        if n == 0:
            pl.semaphore_wait(barrier, count - 1)
        source, owners = span_out[kind], count if kind == "odd" else half
        swap(
            kind,
            opening_order if n == 0 else first_order,
            lambda s: source.at[place[s] % owners],
            span_in.at[n, me],
            source.at[me % owners],
        )
    for load in loads[3:]:
        load.wait()
    cells = float(4 * quarter * 4 * w_ref.shape[1])
    sign = (1 - 2 * (me // half)).astype(jnp.float32)
    for n, kind in enumerate(ORDER):
        arrive(kind, span_in.at[n])
        source, target = back_out[kind], back_in[kind]

        def send():
            if kind == "odd":
                swap(
                    kind + "-back",
                    last_order,
                    lambda s: source.at[place[s]],
                    target.at[me],
                    source.at[me],
                )
            else:
                swap(
                    kind + "-back",
                    beside,
                    lambda s: source.at[place[s] % half],
                    target.at[my_owner],
                    source.at[my_owner],
                )

        stream_stage(
            share,
            py_count,
            my_owner == 0 if kind == "even" else None,
            None if kind == "odd" else sign,
            band_ref,
            span_in.at[n],
            t_h,
            t_l,
            w_ref,
            cells,
            source,
        )
        send()
    groups, _, width, _ = out_ref.shape

    def spread(i, j, value):
        out_ref[:, i, :, j * quarter : (j + 1) * quarter] = value.reshape(groups, width, quarter)

    def spread_more(i, j, value):
        at = slice(j * quarter, (j + 1) * quarter)
        out_ref[:, i, :, at] = out_ref[:, i, :, at] + value.reshape(groups, width, quarter)

    for kind in ("even", "middle"):
        arrive(kind + "-back", back_in[kind], (0,))
        table = [side[...] for side in span_table[kind]]
        keep[kind][...] = back_chunk(share, parts, back_in[kind], table)
    for i in range(parts):
        rows = slice(i * 128, (i + 1) * 128)
        for j in range(2):
            value = keep_even[rows] - keep_middle[rows] if j else keep_even[rows] + keep_middle[rows]
            spread(i, j, value)
            spread(i, j + 2, value)
    side_of_me = me // half
    for steps, side in ((near, side_of_me), (far, 1 - side_of_me)):
        if steps is far:
            for n, kind in enumerate(ORDER):
                sent(kind, span_in.at[n])
            for kind in ("even", "middle"):
                sent(kind + "-back", back_in[kind])
        arrive("odd-back", back_in_odd, (int(steps is far),))
        first = pl.multiple_of(side * half, half)
        wave = pl.multiple_of(side * half * share, half * share)
        table = [
            jnp.concatenate(
                [ref[pl.ds(at + wave, half * share)] for at in (0, quarter)], 0
            )
            for ref in span_table["odd"]
        ]
        source = back_in_odd.at[pl.ds(first, half)]
        both = back_chunk(share, parts, source, table)
        for i in range(parts):
            rows = slice(i * 128, (i + 1) * 128)
            for j in range(4):
                value = both[rows, (j % 2) * quarter : (j % 2 + 1) * quarter]
                spread_more(i, j, value if j < 2 else -value)
    sent("odd-back", back_in_odd)


def register_device(velocity, band_of):
    px_count = lax.axis_size("px")
    py_count = lax.axis_size("py")
    count = px_count * py_count
    _, rows_x, _, span = velocity.shape
    stream = rows_x * px_count
    half, quarter = count // 2, span // 4
    share = quarter // count
    width = stream // count
    groups = 128 // width
    parts = len(PAIR_LIST) * NB // groups
    vmem = pl.BlockSpec(memory_space=pltpu.VMEM)
    far = pl.BlockSpec(memory_space=pltpu.HBM)
    e_h, e_l, m_h, m_l, o_h, o_l = span_tables(span)
    t_h, t_l, twiddle = stream_tables(stream)
    even = [np.concatenate(pair, 1) for pair in ((e_h, m_h), (e_l, m_l))]
    tables = np.concatenate(even + [o_h, o_l, t_h, t_l], 0)
    strips = velocity.size // 128
    rows_in, rows_back = 3 * share, 2 * parts * share
    spans = [(half, rows_in, 128), (half, rows_in, 128), (count, rows_in, 128), (3, count, rows_in, 128)]
    backs = [(n, rows_back, 128) for n in (half, half, count)]
    keeps = [(parts * 128, n * quarter) for n in (1, 1)]
    lanes = 6
    operands = (band_of, velocity.reshape(strips, 128), jnp.asarray(tables), jnp.asarray(twiddle))
    out = pl.pallas_call(
        functools.partial(whole_kernel, px_count, py_count, share, parts),
        out_shape=jax.ShapeDtypeStruct((groups, parts, width, span), jnp.float32),
        in_specs=[far] * 4,
        out_specs=vmem,
        scratch_shapes=[
            pltpu.SMEM(band_of.shape, band_of.dtype),
            pltpu.VMEM((strips, 128), jnp.float32),
            pltpu.VMEM(twiddle.shape, jnp.float32),
            pltpu.VMEM(tables.shape, tables.dtype),
        ]
        + [pltpu.VMEM(shape, jnp.float32) for shape in spans + backs + backs + keeps]
        + [
            pltpu.SemaphoreType.DMA((lanes,)),
            pltpu.SemaphoreType.DMA((lanes, 2)),
            pltpu.SemaphoreType.DMA((6,)),
        ],
        compiler_params=pltpu.CompilerParams(
            collective_id=0, has_side_effects=True, vmem_limit_bytes=49152 * 1024
        ),
    )(*[pltpu.with_memory_space_constraint(value, pltpu.HBM) for value in operands])
    return out.reshape(len(PAIR_LIST), NB, width, span)


def fills_registers(velocity, px_count, py_count):
    comps, rows_x, planes, span = velocity.shape
    count = px_count * py_count
    stream = rows_x * px_count
    share = span // 2 // count
    width = max(stream // count, 1)
    return (
        comps == 3
        and rows_x == 64
        and planes == 1
        and px_count & (px_count - 1) == 0
        and py_count & (py_count - 1) == 0
        and px_count % 8 == 0
        and span % 1024 == 0
        and stream == span
        and stream == width * count
        and planes * py_count == NB
        and NB == 2
        and span == 2 * share * count
        and share == 16
        and width == 32
        and 128 % width == 0
        and len(PAIR_LIST) * NB * width % 128 == 0
    )


def per_device(velocity, band_of):
    if fills_registers(velocity, lax.axis_size("px"), lax.axis_size("py")):
        return register_device(velocity, band_of)
    return general_device(velocity, band_of)


def solution(mesh):
    in_specs = (P(None, "px", "py", None), P())
    out_specs = P(None, None, ("px", "py"), None)
    return jax.shard_map(
        per_device, mesh=mesh, in_specs=in_specs, out_specs=out_specs, check_vma=False
    )
```

```python
import functools
import math

import jax
import jax.numpy as jnp
import numpy as np
from jax import lax
from jax.experimental import pallas as pl
from jax.experimental.pallas import tpu as pltpu
from jax.sharding import PartitionSpec as P

NB = 2


PAIR_LIST = ((0, 0), (0, 1), (0, 2), (1, 1), (1, 2), (2, 2))


def phase_table(row_values, offset, count, length):
    col_values = offset + lax.iota(jnp.int32, count)
    phase = row_values[:, None] * col_values[None, :] % length
    angle = phase.astype(jnp.float32) * (2.0 * math.pi / length)
    return (jnp.cos(angle), jnp.sin(angle))


def transform_last(real_part, imag_part, sign):
    full_shape = real_part.shape
    length = full_shape[-1]
    stacked = jnp.concatenate((real_part.reshape(-1, length), imag_part.reshape(-1, length)), 0)
    row_count = stacked.shape[0] // 2
    row_values = lax.iota(jnp.int32, length)

    def one_block(block_index, outputs):
        offset = (block_index * 128).astype(jnp.int32)
        cosine_table, sine_table = phase_table(row_values, offset, 128, length)
        with_cos = jnp.dot(
            stacked,
            cosine_table,
            precision=lax.Precision.HIGHEST,
            preferred_element_type=jnp.float32,
        )
        with_sin = jnp.dot(
            stacked, sine_table, precision=lax.Precision.HIGHEST, preferred_element_type=jnp.float32
        )
        new_real = with_cos[:row_count] - sign * with_sin[row_count:]
        new_imag = with_cos[row_count:] + sign * with_sin[:row_count]
        return (
            lax.dynamic_update_slice_in_dim(outputs[0], new_real, offset, 1),
            lax.dynamic_update_slice_in_dim(outputs[1], new_imag, offset, 1),
        )

    zeros = jnp.zeros((row_count, length), jnp.float32)
    out_real, out_imag = lax.fori_loop(0, length // 128, one_block, (zeros, zeros))
    return (out_real.reshape(full_shape), out_imag.reshape(full_shape))


def span_forward(velocity):
    comps, rows_x, planes, length = velocity.shape
    half = length // 2
    row_values = lax.iota(jnp.int32, length)

    def one_block(block_index, outputs):
        offset = (block_index * 128).astype(jnp.int32)
        cosine_table, sine_table = phase_table(row_values, offset, 128, length)
        with_cos = jnp.einsum(
            "cxpz,zk->cpkx",
            velocity,
            cosine_table,
            precision=lax.Precision.HIGHEST,
            preferred_element_type=jnp.float32,
        )
        with_sin = jnp.einsum(
            "cxpz,zk->cpkx",
            velocity,
            sine_table,
            precision=lax.Precision.HIGHEST,
            preferred_element_type=jnp.float32,
        )
        return (
            lax.dynamic_update_slice_in_dim(outputs[0], with_cos, offset, 2),
            lax.dynamic_update_slice_in_dim(outputs[1], -with_sin, offset, 2),
        )

    zeros = jnp.zeros((comps, planes, half, rows_x), jnp.float32)
    return lax.fori_loop(0, half // 128, one_block, (zeros, zeros))


def span_inverse(summed, kz_order):
    half = summed.shape[3]
    length = 2 * half
    multiplier = jnp.where(kz_order == 0, 1.0, 2.0).astype(jnp.float32)
    held_real = summed[:, :, 0] * multiplier[:, None]
    held_imag = summed[:, :, 1] * multiplier[:, None]

    def one_block(block_index, output):
        offset = (block_index * 128).astype(jnp.int32)
        cosine_table, sine_table = phase_table(kz_order, offset, 128, length)
        part = jnp.einsum(
            "sbkd,kz->sbdz",
            held_real,
            cosine_table,
            precision=lax.Precision.HIGHEST,
            preferred_element_type=jnp.float32,
        )
        part = part - jnp.einsum(
            "sbkd,kz->sbdz",
            held_imag,
            sine_table,
            precision=lax.Precision.HIGHEST,
            preferred_element_type=jnp.float32,
        )
        return lax.dynamic_update_slice_in_dim(output, part, offset, 3)

    zeros = jnp.zeros((summed.shape[0], summed.shape[1], summed.shape[4], length), jnp.float32)
    return lax.fori_loop(0, length // 128, one_block, zeros)


def general_device(velocity, band_of):
    px_count = lax.axis_size("px")
    py_count = lax.axis_size("py")
    comps, rows_x, planes, span = velocity.shape
    stream = rows_x * px_count
    half = span // 2
    local_k = half // px_count
    span_real, span_imag = span_forward(velocity)
    planes_spec = jnp.stack((span_real, span_imag), 1)
    kz_index = lax.iota(jnp.int32, local_k)
    kx_index = lax.iota(jnp.int32, stream)
    at_anchor = jnp.logical_and(
        lax.axis_index("px") == 0, jnp.logical_and(kz_index[:, None] == 0, kx_index[None, :] == 0)
    )
    keep_mask = 1.0 - at_anchor.astype(jnp.float32)
    received = lax.all_to_all(planes_spec, "px", split_axis=3, concat_axis=4, tiled=True)
    front_real, front_imag = transform_last(received[:, 0], received[:, 1], -1.0)
    spectrum = jnp.stack((front_real * keep_mask, front_imag * keep_mask), 1)
    cross_list = []
    for left_comp, right_comp in PAIR_LIST:
        left_real, left_imag = (spectrum[left_comp, 0], spectrum[left_comp, 1])
        right_real, right_imag = (spectrum[right_comp, 0], spectrum[right_comp, 1])
        cross_list.append(
            jnp.stack(
                (
                    left_real * right_real + left_imag * right_imag,
                    left_real * right_imag - left_imag * right_real,
                ),
                0,
            )
        )
    cross = jnp.stack(cross_list, 0)
    band_ids = lax.iota(jnp.int32, NB)
    onehot_all = (band_of[:, None] == band_ids[None, :]).astype(jnp.float32)
    counts = jnp.sum(onehot_all, 0)
    cells = float(stream * span)
    plane_start = lax.axis_index("py") * planes
    local_hot = lax.dynamic_slice_in_dim(onehot_all, plane_start, planes, 0)
    band_weight = local_hot / (counts[None, :] * (cells * math.sqrt(cells)))
    banded = jnp.einsum("sapkx,pb->sbakx", cross, band_weight, precision=lax.Precision.HIGHEST)
    summed = lax.psum_scatter(banded, "py", scatter_dimension=3, tiled=True)
    back_real, back_imag = transform_last(summed[:, :, 0], summed[:, :, 1], 1.0)
    exchanged = lax.all_to_all(
        lax.all_to_all(
            jnp.stack((back_real, back_imag), 2), "px", split_axis=4, concat_axis=3, tiled=True
        ),
        "py",
        split_axis=4,
        concat_axis=3,
        tiled=True,
    )
    quarter = local_k // py_count
    position = lax.iota(jnp.int32, half)
    outer = position // (px_count * quarter)
    remain = position % (px_count * quarter)
    kz_order = remain // quarter * local_k + outer * quarter + remain % quarter
    return span_inverse(exchanged, kz_order)


def split_table(table):
    high = table.astype(jnp.bfloat16)
    low = (table - high.astype(np.float64)).astype(jnp.bfloat16)
    return high, low


def span_tables(length):
    quarter, eighth = length // 4, length // 8
    column = np.arange(quarter)

    def angle(first, count):
        wave = 4 * np.arange(count) + first
        return 2.0 * np.pi * ((wave[:, None] * column[None, :]) % length) / length

    even = angle(0, eighth)
    middle = angle(2, eighth)
    odd = angle(1, quarter)
    table_even = np.concatenate((np.cos(even), -np.sin(even)), 0)
    table_middle = np.concatenate((np.cos(middle), -np.sin(middle)), 0)
    table_odd = np.block([[np.cos(odd), -np.sin(odd)], [-np.sin(odd), -np.cos(odd)]])
    return split_table(table_even) + split_table(table_middle) + split_table(table_odd)


def stream_tables(length):
    quarter = length // 4
    index = np.arange(quarter)
    angle = 2.0 * np.pi * ((index[:, None] * index[None, :]) % quarter) / quarter
    cosine, sine = np.cos(angle), np.sin(angle)
    twist = 2.0 * np.pi * (np.arange(4)[:, None] * index[None, :]) / length
    twiddle = np.concatenate((np.cos(twist), np.sin(twist)), 0).astype(np.float32)
    return split_table(np.block([[cosine, -sine], [sine, cosine]])) + (twiddle,)


def split_value(value):
    high = value.astype(jnp.bfloat16)
    low = (value - high.astype(jnp.float32)).astype(jnp.bfloat16)
    return high, low


def one_dot(left, right, dims):
    return lax.dot_general(left, right, (dims, ((), ())), preferred_element_type=jnp.float32)


NT = ((1,), (1,))
NN = ((1,), (0,))


def rows_by_table(value, table):
    high, low = split_value(value)
    rows = value.shape[0]
    by_high = one_dot(jnp.concatenate((high, low), 0), table[0], NN)
    return by_high[:rows] + (by_high[rows:] + one_dot(high, table[1], NN))


def table_by_rows(table, value):
    high, low = split_value(value)
    return one_dot(table[0], high, NT) + (
        one_dot(table[1], high, NT) + one_dot(table[0], low, NT)
    )


def span_quarters(v_ref, strips):
    rows = v_ref.shape[0] // strips
    first = rows // 3 * 2

    def strip(j):
        values = v_ref[pl.ds(j, rows, stride=strips), :]
        return jnp.concatenate((values, values[first:]), 0)

    per = strips // 4
    return [
        jnp.concatenate([strip(i * per + n) for n in range(per)], 1) for i in range(4)
    ]


def span_chunk(kind, share, part, table, out_ref):
    if kind == "odd":
        value = jnp.concatenate((part[0] - part[2], part[1] - part[3]), 1)
    else:
        ahead, behind = part[0] + part[2], part[1] + part[3]
        value = ahead + behind if kind == "even" else ahead - behind
    both = table_by_rows((table[0][...], table[1][...]), value)
    count = both.shape[0] // 2
    real, imag = both[:count], both[count:]
    lane = lax.broadcasted_iota(jnp.int32, (count, 128), 1)
    third = jnp.where(lane < 64, real[:, 128:], imag[:, 128:])
    out_ref[:, :share] = real[:, :128].reshape(-1, share, 128)
    out_ref[:, share : 2 * share] = imag[:, :128].reshape(-1, share, 128)
    out_ref[:, 2 * share :] = third.reshape(-1, share, 128)


def lane_exchange(tiles, width):
    tiles = list(tiles)
    lane = lax.broadcasted_iota(jnp.int32, tiles[0].shape, 1)
    step, size = len(tiles) // 2, 64
    while step:
        mask = lane // size % 2 == 0
        for g in range(len(tiles)):
            if g & step == 0:
                a, b = tiles[g], tiles[g + step]
                tiles[g] = jnp.where(mask, a, pltpu.roll(b, size, 1))
                tiles[g + step] = jnp.where(mask, pltpu.roll(a, 128 - size, 1), b)
        step, size = step // 2, size // 2
    return tiles


def stream_stage(share, planes, owns_mean, sign, band_ref, in_ref, t_h, t_l, w_ref, cells, out_ref):
    px_count = in_ref.shape[0] // planes
    columns = px_count // 2
    group_cols = columns // 4
    quarter = w_ref.shape[1]
    lane = lax.broadcasted_iota(jnp.int32, (3 * share, 128), 1)
    low_half = lane < 64
    blocks = []
    for q in range(columns):
        real, imag = [[], [], []], [[], [], []]
        for y in range(planes):
            a = in_ref[2 * q * planes + y]
            b = in_ref[(2 * q + 1) * planes + y]
            low = jnp.where(low_half, a, pltpu.roll(b, 64, 1))
            high = jnp.where(low_half, pltpu.roll(a, 64, 1), b)
            real[0].append(low[:share])
            imag[0].append(low[share : 2 * share])
            real[1].append(high[:share])
            imag[1].append(high[share : 2 * share])
            real[2].append(low[2 * share :])
            imag[2].append(high[2 * share :])
        blocks.append(
            (
                jnp.concatenate(real[0] + real[1] + real[2], 0),
                jnp.concatenate(imag[0] + imag[1] + imag[2], 0),
            )
        )
    part = [
        tuple(
            jnp.concatenate([blocks[j * group_cols + g][ri] for g in range(group_cols)], 1)
            for ri in range(2)
        )
        for j in range(4)
    ]

    def cross4(v):
        s02 = [v[0][i] + v[2][i] for i in range(2)]
        d02 = [v[0][i] - v[2][i] for i in range(2)]
        s13 = [v[1][i] + v[3][i] for i in range(2)]
        d13 = [v[1][i] - v[3][i] for i in range(2)]
        return [
            (s02[0] + s13[0], s02[1] + s13[1]),
            (d02[0] + d13[1], d02[1] - d13[0]),
            (s02[0] - s13[0], s02[1] - s13[1]),
            (d02[0] - d13[1], d02[1] + d13[0]),
        ]

    turned = []
    for k1, (real, imag) in enumerate(cross4(part)):
        if k1:
            cosine, sine = w_ref[k1 : k1 + 1], w_ref[4 + k1 : 5 + k1]
            real, imag = real * cosine + imag * sine, imag * cosine - real * sine
        turned.append(jnp.concatenate((real, imag), 1))
    table = (t_h[...], t_l[...])
    front = rows_by_table(jnp.concatenate(turned, 0), table)
    if owns_mean is not None:
        block = 3 * planes * share
        row = lax.broadcasted_iota(jnp.int32, (block, 2 * quarter), 0)
        col = lax.broadcasted_iota(jnp.int32, (block, 2 * quarter), 1)
        anchor = jnp.logical_and(row % share == 0, col % quarter == 0)
        anchor = jnp.logical_and(anchor, owns_mean)
        front = jnp.concatenate((jnp.where(anchor, 0.0, front[:block]), front[block:]), 0)
    front = front.reshape(4, 3, planes, share, 2 * quarter)
    tall = (4 * share, quarter)

    def spectrum(c, y, ri):
        return front[:, c, y, :, ri * quarter : (ri + 1) * quarter].reshape(tall)

    in_order = jnp.full(tall, band_ref[0], jnp.int32) == 0
    field = [
        [
            tuple(
                jnp.where(in_order, spectrum(c, b, ri), spectrum(c, 1 - b, ri)) for ri in range(2)
            )
            for b in range(NB)
        ]
        for c in range(3)
    ]
    scale = 2.0 / (cells * math.sqrt(cells))
    if owns_mean is not None:
        row = lax.broadcasted_iota(jnp.int32, tall, 0)
        single = jnp.logical_and(row % share == 0, owns_mean)
        scale = jnp.where(single, 0.5 * scale, scale)

    def banded(left, right, b):
        lr, li = field[left][b]
        rr, ri = field[right][b]
        real = (lr * rr + li * ri) * scale
        if left == right:
            return real
        return jnp.concatenate((real, (li * rr - lr * ri) * scale), 1)

    members = list(range(len(PAIR_LIST) * NB))
    lines = [None] * len(members)
    own_table = (t_h[:quarter], t_l[:quarter])
    for alike, used in ((True, own_table), (False, table)):
        chosen = [m for m in members if (len(set(PAIR_LIST[m // NB])) == 1) == alike]
        joined = jnp.concatenate([banded(*PAIR_LIST[m // NB], m % NB) for m in chosen], 0)
        whole = rows_by_table(joined, used)
        for at, m in enumerate(chosen):
            back = whole[at * 4 * share : (at + 1) * 4 * share]
            turned = []
            for k1 in range(4):
                real = back[k1 * share : (k1 + 1) * share, :quarter]
                imag = back[k1 * share : (k1 + 1) * share, quarter:]
                if k1:
                    cosine, sine = w_ref[k1 : k1 + 1], w_ref[4 + k1 : 5 + k1]
                    if sign is not None and k1 % 2:
                        cosine, sine = cosine * sign, sine * sign
                    real, imag = real * cosine + imag * sine, imag * cosine - real * sine
                turned.append((real, imag))
            lines[m] = cross4(turned)
    held = 4 * quarter if sign is None else 2 * quarter
    width = held // out_ref.shape[0]
    groups = 128 // width
    per_group = len(members) // groups
    for i in range(per_group):
        for ri in range(2):
            at = (i * 2 + ri) * share
            for q in range(held // 128):
                j, inside = q * 128 // quarter, q * 128 % quarter
                tiles = [
                    lines[g * per_group + i][j][ri][:, inside : inside + 128]
                    for g in range(groups)
                ]
                for t, packed in enumerate(lane_exchange(tiles, width)):
                    out_ref[q * groups + t, at : at + share] = packed


def back_chunk(share, parts, in_ref, table):
    sources = in_ref.shape[0]

    def turned(i, ri):
        at = (i * 2 + ri) * share
        return in_ref[:, at : at + share].reshape(sources * share, 128).T

    value = jnp.concatenate(
        [jnp.concatenate((turned(i, 0), -turned(i, 1)), 1) for i in parts], 0
    )
    return rows_by_table(value, table)


def flip_bits(index, bits):
    moved, bit = index, 1
    while bit <= bits:
        if bits & bit:
            moved = moved + bit * (1 - 2 * ((index // bit) % 2))
        bit *= 2
    return moved


ORDER = ("even", "odd", "middle")
SEND_ORDER = "fx xx fn nd"


def whole_kernel(
    px_count,
    py_count,
    share,
    parts,
    band_far,
    v_far,
    table_far,
    w_far,
    out_ref,
    band_ref,
    v_ref,
    w_ref,
    tables,
    span_out_even,
    span_out_middle,
    span_out_odd,
    span_in,
    back_out_even,
    back_out_middle,
    back_out_odd,
    back_in_even,
    back_in_middle,
    back_in_odd,
    keep_even,
    keep_middle,
    send_sem,
    recv_sem,
    load_sem,
):
    quarter = tables.shape[1] // 2
    cuts = (0, 2 * quarter, 6 * quarter, 10 * quarter)
    pairs = [(v_far, v_ref)]
    pairs += [
        (table_far.at[start:stop], tables.at[start:stop])
        for start, stop in zip(cuts[:-1], cuts[1:])
    ]
    pairs += [(w_far, w_ref), (band_far, band_ref)]
    loads = [
        pltpu.make_async_copy(source, target, load_sem.at[n])
        for n, (source, target) in enumerate(pairs)
    ]
    span_table = {
        "even": [tables.at[n * quarter : (n + 1) * quarter, :quarter] for n in range(2)],
        "middle": [tables.at[n * quarter : (n + 1) * quarter, quarter:] for n in range(2)],
        "odd": [tables.at[n * quarter : (n + 2) * quarter] for n in (2, 4)],
    }
    t_h, t_l = tables.at[6 * quarter : 8 * quarter], tables.at[8 * quarter :]
    px, py = lax.axis_index("px"), lax.axis_index("py")
    count = px_count * py_count
    half = count // 2
    me = px * py_count + py
    my_owner = me % half
    barrier = pltpu.get_barrier_semaphore()
    near, far = list(range(1, half)), list(range(half, count))
    peers = {
        s: (flip_bits(px, s // py_count), flip_bits(py, s % py_count)) for s in near + far
    }
    place = {s: peers[s][0] * py_count + peers[s][1] for s in peers}
    for s in far + near:
        pl.semaphore_signal(
            barrier, inc=1, device_id=peers[s], device_id_type=pl.DeviceIdType.MESH
        )
    for load in loads:
        load.start()
    moves = {}

    def swap(name, steps, source_at, target, own_source):
        lane = len(moves)
        for s in steps:
            pltpu.make_async_remote_copy(
                src_ref=source_at(s),
                dst_ref=target,
                send_sem=send_sem.at[lane],
                recv_sem=recv_sem.at[lane, int(s >= half)],
                device_id=peers[s],
                device_id_type=pl.DeviceIdType.MESH,
            ).start()
        pltpu.make_async_copy(own_source, target, recv_sem.at[lane, 0]).start()
        moves[name] = (lane, len(steps))

    def arrive(name, into, sides=(0, 1)):
        for side in sides:
            slots = into.at[:half]
            pltpu.make_async_copy(slots, slots, recv_sem.at[moves[name][0], side]).wait()

    def sent(name, into):
        lane, copies = moves[name]
        slots = into.at[:copies]
        pltpu.make_async_copy(slots, slots, send_sem.at[lane]).wait()

    orders = {
        "nf": near + far,
        "fn": far + near,
        "dn": (near + far)[::-1],
        "nu": near,
        "nd": near[::-1],
        "xx": near[::-1] + far[::-1],
        "fx": far[::-1] + near[::-1],
    }
    opening_order, first_order, last_order, beside = (
        orders[name] for name in SEND_ORDER.split()
    )
    span_out = {"even": span_out_even, "middle": span_out_middle, "odd": span_out_odd}
    back_out = {"even": back_out_even, "middle": back_out_middle, "odd": back_out_odd}
    back_in = {"even": back_in_even, "middle": back_in_middle, "odd": back_in_odd}
    keep = {"even": keep_even, "middle": keep_middle}
    loads[0].wait()
    part = span_quarters(v_ref, 4 * quarter // 128)
    for n, kind in enumerate(ORDER):
        if n == 0 or (kind == "odd") != (ORDER[n - 1] == "odd"):
            at = 2 if kind == "odd" else 1
            if loads[at] is not None:
                loads[at].wait()
                loads[at] = None
        span_chunk(kind, share, part, span_table[kind], span_out[kind])
        if n == 0:
            pl.semaphore_wait(barrier, count - 1)
        source, owners = span_out[kind], count if kind == "odd" else half
        swap(
            kind,
            opening_order if n == 0 else first_order,
            lambda s: source.at[place[s] % owners],
            span_in.at[n, me],
            source.at[me % owners],
        )
    for load in loads[3:]:
        load.wait()
    cells = float(4 * quarter * 4 * w_ref.shape[1])
    sign = (1 - 2 * (me // half)).astype(jnp.float32)
    for n, kind in enumerate(ORDER):
        arrive(kind, span_in.at[n])
        source, target = back_out[kind], back_in[kind]

        def send():
            if kind == "odd":
                swap(
                    kind + "-back",
                    last_order,
                    lambda s: source.at[place[s]],
                    target.at[me],
                    source.at[me],
                )
            else:
                swap(
                    kind + "-back",
                    beside,
                    lambda s: source.at[place[s] % half],
                    target.at[my_owner],
                    source.at[my_owner],
                )

        stream_stage(
            share,
            py_count,
            my_owner == 0 if kind == "even" else None,
            None if kind == "odd" else sign,
            band_ref,
            span_in.at[n],
            t_h,
            t_l,
            w_ref,
            cells,
            source,
        )
        send()
    groups, _, width, _ = out_ref.shape

    def spread(i, j, value):
        out_ref[:, i, :, j * quarter : (j + 1) * quarter] = value.reshape(groups, width, quarter)

    def spread_more(i, j, value):
        at = slice(j * quarter, (j + 1) * quarter)
        out_ref[:, i, :, at] = out_ref[:, i, :, at] + value.reshape(groups, width, quarter)

    for kind in ("even", "middle"):
        arrive(kind + "-back", back_in[kind], (0,))
        table = [side[...] for side in span_table[kind]]
        keep[kind][...] = back_chunk(share, range(parts), back_in[kind], table)
    for i in range(parts):
        rows = slice(i * 128, (i + 1) * 128)
        for j in range(2):
            value = keep_even[rows] - keep_middle[rows] if j else keep_even[rows] + keep_middle[rows]
            spread(i, j, value)
            spread(i, j + 2, value)
    side_of_me = me // half
    for steps, side in ((near, side_of_me), (far, 1 - side_of_me)):
        if steps is far:
            for n, kind in enumerate(ORDER):
                sent(kind, span_in.at[n])
            for kind in ("even", "middle"):
                sent(kind + "-back", back_in[kind])
        arrive("odd-back", back_in_odd, (int(steps is far),))
        first = pl.multiple_of(side * half, half)
        wave = pl.multiple_of(side * half * share, half * share)
        table = [
            jnp.concatenate(
                [ref[pl.ds(at + wave, half * share)] for at in (0, quarter)], 0
            )
            for ref in span_table["odd"]
        ]
        source = back_in_odd.at[pl.ds(first, half)]
        for i in range(parts):
            both = back_chunk(share, [i], source, table)
            for j in range(4):
                value = both[:, (j % 2) * quarter : (j % 2 + 1) * quarter]
                spread_more(i, j, value if j < 2 else -value)
    sent("odd-back", back_in_odd)


def register_device(velocity, band_of):
    px_count = lax.axis_size("px")
    py_count = lax.axis_size("py")
    count = px_count * py_count
    _, rows_x, _, span = velocity.shape
    stream = rows_x * px_count
    half, quarter = count // 2, span // 4
    share = quarter // count
    width = stream // count
    groups = 128 // width
    parts = len(PAIR_LIST) * NB // groups
    vmem = pl.BlockSpec(memory_space=pltpu.VMEM)
    far = pl.BlockSpec(memory_space=pltpu.HBM)
    e_h, e_l, m_h, m_l, o_h, o_l = span_tables(span)
    t_h, t_l, twiddle = stream_tables(stream)
    even = [np.concatenate(pair, 1) for pair in ((e_h, m_h), (e_l, m_l))]
    tables = np.concatenate(even + [o_h, o_l, t_h, t_l], 0)
    strips = velocity.size // 128
    rows_in, rows_back = 3 * share, 2 * parts * share
    spans = [(half, rows_in, 128), (half, rows_in, 128), (count, rows_in, 128), (3, count, rows_in, 128)]
    backs = [(n, rows_back, 128) for n in (half, half, count)]
    keeps = [(parts * 128, n * quarter) for n in (1, 1)]
    lanes = 6
    operands = (band_of, velocity.reshape(strips, 128), jnp.asarray(tables), jnp.asarray(twiddle))
    out = pl.pallas_call(
        functools.partial(whole_kernel, px_count, py_count, share, parts),
        out_shape=jax.ShapeDtypeStruct((groups, parts, width, span), jnp.float32),
        in_specs=[far] * 4,
        out_specs=vmem,
        scratch_shapes=[
            pltpu.SMEM(band_of.shape, band_of.dtype),
            pltpu.VMEM((strips, 128), jnp.float32),
            pltpu.VMEM(twiddle.shape, jnp.float32),
            pltpu.VMEM(tables.shape, tables.dtype),
        ]
        + [pltpu.VMEM(shape, jnp.float32) for shape in spans + backs + backs + keeps]
        + [
            pltpu.SemaphoreType.DMA((lanes,)),
            pltpu.SemaphoreType.DMA((lanes, 2)),
            pltpu.SemaphoreType.DMA((6,)),
        ],
        compiler_params=pltpu.CompilerParams(
            collective_id=0, has_side_effects=True, vmem_limit_bytes=49152 * 1024
        ),
    )(*[pltpu.with_memory_space_constraint(value, pltpu.HBM) for value in operands])
    return out.reshape(len(PAIR_LIST), NB, width, span)


def fills_registers(velocity, px_count, py_count):
    comps, rows_x, planes, span = velocity.shape
    count = px_count * py_count
    stream = rows_x * px_count
    share = span // 2 // count
    width = max(stream // count, 1)
    return (
        comps == 3
        and rows_x == 64
        and planes == 1
        and px_count & (px_count - 1) == 0
        and py_count & (py_count - 1) == 0
        and px_count % 8 == 0
        and span % 1024 == 0
        and stream == span
        and stream == width * count
        and planes * py_count == NB
        and NB == 2
        and span == 2 * share * count
        and share == 16
        and width == 32
        and 128 % width == 0
        and len(PAIR_LIST) * NB * width % 128 == 0
    )


def per_device(velocity, band_of):
    if fills_registers(velocity, lax.axis_size("px"), lax.axis_size("py")):
        return register_device(velocity, band_of)
    return general_device(velocity, band_of)


def solution(mesh):
    in_specs = (P(None, "px", "py", None), P())
    out_specs = P(None, None, ("px", "py"), None)
    return jax.shard_map(
        per_device, mesh=mesh, in_specs=in_specs, out_specs=out_specs, check_vma=False
    )
```
